32 devices in a mesh: grp: 4 (over y, core), dom: 8 (over z, x).
Axes of the slice: x: 2, y: 2, z: 4, core: 2. Of those that a mesh axis runs over, the one named last changes fastest.
Arguments:
- fine_nodes: bfloat16 [4, 6144, 128], P('grp', 'dom'), may hold values from -6 to 6
- fine_edges: bfloat16 [4, 73728, 128], P('grp', 'dom'), may hold values from -6 to 6
- fine_senders: int32 [4, 73728], P('grp', 'dom'), may hold values from 0 to 959
- fine_receivers: int32 [4, 73728], P('grp', 'dom'), may hold values from 0 to 767, as said below
- edge_count: int32 [4, 8], P('grp', 'dom'), may hold values from 4608 to 9216, as said below
- ghost_send: int32 [4, 64, 24], P('grp', 'dom'), may hold values from 0 to 767
- fine_parent: int32 [4, 6144], P('grp', 'dom'), may hold values from 0 to 4095, as said below
- coarse_nodes: bfloat16 [4096, 128], P('dom'), may hold values from -6 to 6
- coarse_edges: bfloat16 [32768, 128], P('dom'), may hold values from -6 to 6
- coarse_senders: int32 [32768], P('dom'), may hold values from 0 to 4095
- coarse_receivers: int32 [32768], P('dom'), may hold values from 0 to 511, as said below
- edge_in: bfloat16 [2, 384, 128], replicated, may hold values from -0.3125 to 0.3125
- node_in: bfloat16 [3, 256, 128], replicated, may hold values from -0.375 to 0.375
- mlp_out: bfloat16 [5, 128, 128], replicated, may hold values from -0.5 to 0.5
Outputs:
- fine_out: bfloat16 [4, 6144, 128], P('grp', 'dom')
- coarse_out: bfloat16 [4096, 128], P('dom')
The draws below stay inside these ranges and needn't reach their ends.
Inputs may be any that keep to these rules, and one draw needn't show every extreme that they name: `edge_count`: each device's live edge slot count; slots from that count on are padding; 9216 on at least one device. `fine_receivers`: nondecreasing along each device's 9216 slots; padding slots hold 767. `fine_senders`: below 768: a local node; 768 + s * 24 + k: ghost slot k received from dom index s of the same slab. `ghost_send`: local node indices; row p of a device's block lists the nodes sent to dom index p. `fine_parent`: global coarse index; owner o holds coarse nodes o * 512 to (o + 1) * 512 - 1. Most parents of a fine node of dom index d are owned by d itself; the others may be owned by any owner. `coarse_senders`: global coarse index of the sender. `coarse_receivers`: nondecreasing within each owner's 4096 edges.
All inputs are finite; a program needn't handle non-finite values.
Results may differ from the reference program's by a relative error of at most 0.015.
Values may be sent and summed in bfloat16 or wider, within the bound.
No kernel may reach another device: no remote copies, remote signals or barrier semaphores. Data moves between devices by JAX's collectives and lax.ppermute only.
A program may use at most 64 MiB of HBM per device.

```python
import jax
import jax.numpy as jnp
from jax import lax

L = 128
NF_DEV = 768
C_DEV = 512
E_DEV = 9216
GH = 24
EC_DEV = 4096
COARSE = 4096
N_GRP = 4
N_DOM = 8


def ragged_edges(key):
    folded = jax.random.fold_in(key, 11)
    first, second, third = jax.random.split(folded, 3)
    counts = jax.random.randint(first, (N_GRP * N_DOM,), E_DEV // 2, E_DEV + 1)
    chosen = jax.random.randint(third, (), 0, N_GRP * N_DOM)
    counts = counts.at[chosen].set(E_DEV).astype(jnp.int32)
    base = jnp.sort(jax.random.randint(second, (N_GRP * N_DOM, E_DEV), 0, NF_DEV), axis=-1)
    slots = jnp.arange(E_DEV, dtype=jnp.int32)
    position = jnp.minimum(slots[None, :] * E_DEV // counts[:, None], E_DEV - 1)
    picked = jnp.take_along_axis(base, position, axis=-1)
    receivers = jnp.where(slots[None, :] < counts[:, None], picked, NF_DEV - 1)
    return (counts.reshape(N_GRP, N_DOM), receivers.reshape(N_GRP, N_DOM * E_DEV).astype(jnp.int32))


def draw_edge_count(key, part):
    return ragged_edges(key)[0]


def draw_fine_receivers(key, part):
    return ragged_edges(key)[1]


def draw_fine_parent(key, part):
    folded = jax.random.fold_in(key, 37)
    first, second, third = jax.random.split(folded, 3)
    shape = (N_GRP, N_DOM * NF_DEV)
    position = jnp.arange(N_DOM * NF_DEV, dtype=jnp.int32)
    domain = (position // NF_DEV)[None, :]
    spill = jax.random.randint(first, shape, 0, 100) < 25
    offset = jax.random.randint(second, shape, 1, N_DOM)
    offset = jnp.where(spill, offset, 0)
    offset = jnp.where((position % NF_DEV == 0)[None, :], N_DOM // 2, offset)
    owner = (domain + offset) % N_DOM
    within = jax.random.randint(third, shape, 0, C_DEV)
    return (owner * C_DEV + within).astype(jnp.int32)


def draw_coarse_receivers(key, part):
    folded = jax.random.fold_in(key, 23)
    raw = jax.random.randint(folded, (N_DOM, EC_DEV), 0, C_DEV)
    return jnp.sort(raw, axis=-1).reshape(N_DOM * EC_DEV).astype(jnp.int32)


def plant(values, own_key, smallest, largest):
    longest = values.shape.index(max(values.shape))
    spots = []
    for shift in (0, 1):
        where = [jax.random.randint(jax.random.fold_in(own_key, axis), (), 0, length) for axis, length in enumerate(values.shape)]
        where[longest] = (where[longest] + shift) % values.shape[longest]
        spots.append(tuple(where))
    return values.at[spots[0]].set(smallest).at[spots[1]].set(largest)


def block_scale(own_key, dims, pieces, low, largest):
    level = 1.0
    for axis_at, shards_of in pieces:
        draws = jax.random.uniform(jax.random.fold_in(jax.random.fold_in(own_key, 6), axis_at), (shards_of,), jnp.float32, low / len(pieces), largest / len(pieces))
        level = level * jnp.repeat(jnp.exp(draws), dims[axis_at] // shards_of).reshape((-1,) + (1,) * (len(dims) - 1 - axis_at))
    return level


def scatter_about(rng, shape, deviation, limit, cuts=(), kind=jnp.bfloat16):
    array = deviation * jax.random.normal(rng, shape, jnp.float32)
    if cuts:
        array = array * block_scale(rng, shape, cuts, -0.22, 0.18)
    return jnp.clip(array, -limit, limit).astype(kind)


def setup_inputs(seed: int = 0) -> dict:
    key_list = jax.random.split(jax.random.key(seed), 15)
    fine_nodes = scatter_about(key_list[0], (N_GRP, N_DOM * NF_DEV, L), 1.0, 6.0, ((0, 4), (1, 8)))
    fine_edges = scatter_about(key_list[1], (N_GRP, N_DOM * E_DEV, L), 1.0, 6.0, ((0, 4), (1, 8)))
    fine_senders = plant(jax.random.randint(key_list[2], (N_GRP, N_DOM * E_DEV), 0, NF_DEV + N_DOM * GH), jax.random.fold_in(key_list[2], 1), 0, (NF_DEV + N_DOM * GH) - 1).astype(jnp.int32)
    fine_receivers = draw_fine_receivers(jax.random.fold_in(key_list[14], 71), 0)
    edge_count = draw_edge_count(jax.random.fold_in(key_list[14], 71), 0)
    ghost_send = plant(jax.random.randint(key_list[5], (N_GRP, N_DOM * N_DOM, GH), 0, NF_DEV), jax.random.fold_in(key_list[5], 1), 0, NF_DEV - 1).astype(jnp.int32)
    fine_parent = draw_fine_parent(jax.random.fold_in(key_list[14], 71), 0)
    coarse_nodes = scatter_about(key_list[7], (COARSE, L), 1.0, 6.0, ((0, 8),))
    coarse_edges = scatter_about(key_list[8], (N_DOM * EC_DEV, L), 1.0, 6.0, ((0, 8),))
    coarse_senders = plant(jax.random.randint(key_list[9], (N_DOM * EC_DEV,), 0, COARSE), jax.random.fold_in(key_list[9], 1), 0, COARSE - 1).astype(jnp.int32)
    coarse_receivers = draw_coarse_receivers(jax.random.fold_in(key_list[14], 71), 0)
    edge_in = scatter_about(key_list[11], (2, 3 * L, L), (3 * L) ** -0.5, 0.3125)
    node_in = scatter_about(key_list[12], (3, 2 * L, L), (2 * L) ** -0.5, 0.375)
    mlp_out = scatter_about(key_list[13], (5, L, L), L ** -0.5, 0.5)
    return dict(fine_nodes=fine_nodes, fine_edges=fine_edges, fine_senders=fine_senders, fine_receivers=fine_receivers, edge_count=edge_count, ghost_send=ghost_send, fine_parent=fine_parent, coarse_nodes=coarse_nodes, coarse_edges=coarse_edges, coarse_senders=coarse_senders, coarse_receivers=coarse_receivers, edge_in=edge_in, node_in=node_in, mlp_out=mlp_out)


def layer_norm(values):
    centre = values - lax.optimization_barrier(jnp.mean(values, -1, keepdims=True))
    spread = lax.optimization_barrier(jnp.mean(centre * centre, -1, keepdims=True))
    return centre * lax.rsqrt(spread + 1e-05)

def perceptron(inputs, w_first, w_second):
    hidden = jax.nn.silu(jnp.dot(inputs, w_first, preferred_element_type=jnp.float32)).astype(jnp.bfloat16)
    return layer_norm(jnp.dot(hidden, w_second, preferred_element_type=jnp.float32))

def reference(fine_nodes, fine_edges, fine_senders, fine_receivers, edge_count, ghost_send, fine_parent, coarse_nodes, coarse_edges, coarse_senders, coarse_receivers, edge_in, node_in, mlp_out):
    devices_all = N_GRP * N_DOM
    nodes_all = fine_nodes.reshape(N_GRP, N_DOM, NF_DEV, L)
    edges_all = fine_edges.reshape(devices_all, E_DEV, L)
    senders_all = fine_senders.reshape(devices_all, E_DEV)
    receivers_all = fine_receivers.reshape(devices_all, E_DEV)
    counts_all = edge_count.reshape(devices_all)
    sends_all = ghost_send.reshape(N_GRP, N_DOM, N_DOM, GH)
    parents_all = fine_parent.reshape(devices_all, NF_DEV)
    peers = jnp.arange(N_DOM)

    def fine_step(index):
        group = index // N_DOM
        domain = index % N_DOM
        local = nodes_all[group, domain]
        picks = sends_all[group, :, domain, :]
        ghosts = nodes_all[group][peers[:, None], picks]
        table = jnp.concatenate([local, ghosts.reshape(N_DOM * GH, L)], 0)
        edges = edges_all[index]
        receivers = receivers_all[index]
        inputs = jnp.concatenate([edges, local[receivers], table[senders_all[index]]], -1)
        edge_new = edges.astype(jnp.float32) + perceptron(inputs, edge_in[0], mlp_out[0])
        live = (jnp.arange(E_DEV) < counts_all[index]).astype(jnp.float32)
        summed = jax.ops.segment_sum(edge_new * live[:, None], receivers, num_segments=NF_DEV).astype(jnp.bfloat16)
        node_new = local.astype(jnp.float32) + perceptron(jnp.concatenate([local, summed], -1), node_in[0], mlp_out[1])
        return node_new.astype(jnp.bfloat16)
    fine_mid = lax.map(fine_step, jnp.arange(devices_all))
    flat_parent = parents_all.reshape(-1)
    pooled = jax.ops.segment_sum(fine_mid.reshape(-1, L).astype(jnp.float32), flat_parent, num_segments=COARSE)
    children = jax.ops.segment_sum(jnp.ones(flat_parent.shape, jnp.float32), flat_parent, num_segments=COARSE)
    coarse_mid = ((coarse_nodes.astype(jnp.float32) + pooled) / (1.0 + children)[:, None]).astype(jnp.bfloat16)
    cedges_all = coarse_edges.reshape(N_DOM, EC_DEV, L)
    csend_all = coarse_senders.reshape(N_DOM, EC_DEV)
    crecv_all = coarse_receivers.reshape(N_DOM, EC_DEV)
    cmid_all = coarse_mid.reshape(N_DOM, C_DEV, L)

    def coarse_step(owner):
        own = cmid_all[owner]
        cedges = cedges_all[owner]
        receivers = crecv_all[owner]
        inputs = jnp.concatenate([cedges, own[receivers], coarse_mid[csend_all[owner]]], -1)
        cedge_new = cedges.astype(jnp.float32) + perceptron(inputs, edge_in[1], mlp_out[2])
        summed = jax.ops.segment_sum(cedge_new, receivers, num_segments=C_DEV).astype(jnp.bfloat16)
        updated = own.astype(jnp.float32) + perceptron(jnp.concatenate([own, summed], -1), node_in[1], mlp_out[3])
        return updated.astype(jnp.bfloat16)
    coarse_out = lax.map(coarse_step, jnp.arange(N_DOM)).reshape(COARSE, L)

    def return_step(index):
        middle = fine_mid[index]
        above = coarse_out[parents_all[index]]
        updated = middle.astype(jnp.float32) + perceptron(jnp.concatenate([middle, above], -1), node_in[2], mlp_out[4])
        return updated.astype(jnp.bfloat16)
    fine_out = lax.map(return_step, jnp.arange(devices_all)).reshape(N_GRP, N_DOM * NF_DEV, L)
    return (fine_out, coarse_out)
```

```python
import functools

import jax
import jax.numpy as jnp
from jax import lax
from jax.experimental import pallas as pl
from jax.experimental.pallas import tpu as pltpu
from jax.sharding import PartitionSpec as P

F32 = jnp.float32
BF16 = jnp.bfloat16
NT = (((1,), (1,)), ((), ()))
CHUNK = 256
LANES = 128
VMEM = pl.BlockSpec(memory_space=pltpu.VMEM)
SMEM = pl.BlockSpec(memory_space=pltpu.SMEM)


def log2(n):
    bits = n.bit_length() - 1
    assert 1 << bits == n
    return bits


def mm(a, b):
    return jnp.dot(a, b, preferred_element_type=F32)


def mm_nt(a, b):
    return lax.dot_general(a, b, NT, preferred_element_type=F32)


def turn(w):
    return w.astype(F32).T.astype(BF16)


def silu(v):
    u = 0.5 * v
    return (u + u * jnp.tanh(u)).astype(BF16)


def norm(y, axis):
    centre = y - jnp.mean(y, axis, keepdims=True)
    spread = jnp.mean(centre * centre, axis, keepdims=True)
    return centre * lax.rsqrt(spread + 1e-05)


def mlp_rows(first, w_second):
    return norm(mm(silu(first), w_second), 1)


def steps(rows):
    base = lax.broadcasted_iota(jnp.int32, (16, LANES), 0)
    return [(base + 16 * j).astype(F32).astype(BF16) for j in range(rows // 16)]


def hot(row, base, blocks):
    rows = 16 * len(blocks)
    n = row.shape[1]
    near = jnp.clip(jnp.broadcast_to(row, (16, n)) - base, -1, rows).astype(F32).astype(BF16)
    one = jnp.ones((16, n), BF16)
    zero = jnp.zeros((16, n), BF16)
    return jnp.concatenate(
        [jnp.where(jnp.concatenate([b] * (n // LANES), 1) == near, one, zero) for b in blocks], 0
    )


def ghosts_kernel(send, local, out, wide, picked):
    wide[...] = local[...].astype(F32)
    peers, slots = send.shape

    def one(p, _):
        for k in range(slots):
            picked[pl.ds(p * slots + k, 1), :] = wide[pl.ds(send[p, k], 1), :]
        return 0

    lax.fori_loop(0, peers, one, 0)
    out[...] = picked[...].astype(BF16)


def fine_kernel(
    count, bounds, edges, senders, receivers, local, ghosts, parents, w_edge, w_node, w_out,
    out, tab, rec, pre, agg, mix, second,
):
    step = pl.program_id(0)
    tile, width = edges.shape
    nodes = local.shape[0]
    table_rows = nodes + ghosts.shape[0]
    chunks = tab.shape[0]
    windows = rec.shape[0]
    blocks = steps(CHUNK)

    @pl.when(step == 0)
    def _():
        w = w_edge[...]
        w_self = turn(w[:width])
        w_recv = turn(w[width : 2 * width])
        w_send = turn(w[2 * width :])
        eye = (
            lax.broadcasted_iota(jnp.int32, (width, width), 0)
            == lax.broadcasted_iota(jnp.int32, (width, width), 1)
        ).astype(F32).astype(BF16)
        mix[...] = jnp.concatenate([w_self, eye], 0)
        second[...] = turn(w_out[0])
        mine = local[...]
        for c in range(windows):
            rec[c] = mm_nt(w_recv, mine[c * CHUNK : (c + 1) * CHUNK]).astype(BF16)
        whole = jnp.concatenate([mine, ghosts[...]], 0)
        extra = chunks * CHUNK - table_rows
        if extra:
            whole = jnp.concatenate([whole, jnp.zeros((extra, width), BF16)], 0)
        for c in range(chunks):
            tab[c] = mm_nt(w_send, whole[c * CHUNK : (c + 1) * CHUNK]).astype(BF16)
        agg[...] = jnp.zeros_like(agg)

    live = count[0, 0]

    @pl.when(step * tile < live)
    def _():
        row = senders[...]
        both = mm_nt(mix[...], edges[...])
        first = both[:width]
        for c in range(chunks):
            first += mm(tab[c], hot(row, c * CHUNK, blocks))
        pre[...] = first
        slots = step * tile + lax.broadcasted_iota(jnp.int32, (1, tile), 1)
        to = jnp.where(slots < live, receivers[...], -1)
        low = bounds[0, 0]
        high = bounds[0, tile - 1]

        def inside(c):
            return (low < (c + 1) * CHUNK) & (high >= c * CHUNK)

        for c in range(windows):

            @pl.when(inside(c))
            def _():
                pre[...] += mm(rec[c], hot(to, c * CHUNK, blocks))

        y = mm(second[...], silu(pre[...]))
        new = (both[width:] + norm(y, 0)).astype(BF16)
        for c in range(windows):

            @pl.when(inside(c))
            def _():
                agg[pl.ds(c * CHUNK, CHUNK), :] += mm_nt(hot(to, c * CHUNK, blocks), new)

    @pl.when(step == pl.num_programs(0) - 1)
    def _():
        mine = local[...]
        w = w_node[0]
        first = mm(mine, w[:width]) + mm(agg[...].astype(BF16), w[width:])
        out[pl.ds(0, nodes), :] = (mine.astype(F32) + mlp_rows(first, w_out[1])).astype(BF16)
        ids = parents[...]
        lines = nodes // LANES
        pads = out.shape[0] - nodes - 2 * lines
        parts = [ids[:, j * LANES : (j + 1) * LANES] for j in range(lines)]
        digits = [p >> 6 for p in parts] + [p & 63 for p in parts]
        digits = digits + [jnp.zeros((1, LANES), jnp.int32)] * pads
        out[pl.ds(nodes, 2 * lines + pads), :] = jnp.concatenate(digits, 0).astype(F32).astype(BF16)


def place(ids, owner_rows, piece, domains, group):
    owner = ids >> log2(owner_rows)
    within = ids & (owner_rows - 1)
    return (within >> log2(piece)) ^ group, owner * piece + (within & (piece - 1))


def pool_kernel(*refs, owner_rows, piece, domains, nodes):
    packs, out = refs[:-1], refs[-1]
    group = lax.axis_index("grp")
    lines = nodes // LANES
    blocks = steps(CHUNK)
    width = out.shape[1]
    chunk_rows = piece + 16
    spots = []
    fulls = []
    for pack in packs:
        tail = pack[pl.ds(nodes, pack.shape[0] - nodes), :].astype(F32).astype(jnp.int32)
        ids = jnp.concatenate(
            [(tail[j : j + 1] << 6) + tail[lines + j : lines + j + 1] for j in range(lines)], 1
        )
        side, spot = place(ids, owner_rows, piece, domains, group)
        spots.append(jnp.where(side == 0, spot, -1))
        fulls.append(
            jnp.concatenate([pack[pl.ds(0, nodes), :], jnp.ones((nodes, LANES), BF16)], 1)
        )
    eye = lax.broadcasted_iota(jnp.int32, (piece, LANES), 0) == lax.broadcasted_iota(
        jnp.int32, (piece, LANES), 1
    )
    lane_row = lax.broadcasted_iota(jnp.int32, (16, LANES), 0)
    for c in range(domains * piece // CHUNK):
        total = mm(hot(spots[0], c * CHUNK, blocks), fulls[0])
        for spot, full in zip(spots[1:], fulls[1:]):
            total += mm(hot(spot, c * CHUNK, blocks), full)
        for q in range(CHUNK // piece):
            base = (c * CHUNK // piece + q) * chunk_rows
            part = total[q * piece : (q + 1) * piece]
            out[pl.ds(base, piece), :] = part[:, :width].astype(BF16)
            many = jnp.sum(jnp.where(eye, part[:, width:], 0.0), 0, keepdims=True)
            high = jnp.floor(many * (1.0 / 256.0))
            low = many - 256.0 * high
            both = jnp.where(lane_row == 0, high, jnp.where(lane_row == 1, low, 0.0))
            out[pl.ds(base + piece, 16), :] = both.astype(BF16)


def coarse_mid_kernel(got, nodes, out, *, piece, domains):
    group = lax.axis_index("grp")
    chunk_rows = piece + 16
    parts = [got[pl.ds(s * chunk_rows, chunk_rows), :].astype(F32) for s in range(domains)]
    total = functools.reduce(jnp.add, parts)
    row = 256.0 * total[piece : piece + 1] + total[piece + 1 : piece + 2]
    eye = lax.broadcasted_iota(jnp.int32, (piece, LANES), 0) == lax.broadcasted_iota(
        jnp.int32, (piece, LANES), 1
    )
    many = jnp.sum(jnp.where(eye, jnp.broadcast_to(row, (piece, LANES)), 0.0), 1, keepdims=True)
    start = pl.multiple_of(group * piece, piece)
    mine = nodes[pl.ds(start, piece), :].astype(F32)
    mid = ((mine + total[:piece]) / (1.0 + many)).astype(BF16)
    for s in range(domains):
        out[pl.ds(s * piece, piece), :] = mid


def fill_table(parts, w, tab):
    per = parts[0].shape[0] // CHUNK
    for k, part in enumerate(parts):
        for c in range(per):
            tab[k * per + c] = mm_nt(w, part[pl.ds(c * CHUNK, CHUNK), :]).astype(BF16)


def coarse_kernel(
    *refs, groups, owner_rows, piece, domains, tile
):
    parts = refs[:groups]
    edges, senders, receivers, w_edge, w_node, w_out = refs[groups : groups + 6]
    out, tab, agg = refs[groups + 6 :]
    group = lax.axis_index("grp")
    domain = lax.axis_index("dom")
    width = edges.shape[1]
    blocks = steps(CHUNK)
    small = steps(piece)
    w = w_edge[1]
    eye = (
        lax.broadcasted_iota(jnp.int32, (width, width), 0)
        == lax.broadcasted_iota(jnp.int32, (width, width), 1)
    ).astype(F32).astype(BF16)
    mix = jnp.concatenate([turn(w[:width]), eye], 0)
    fill_table(parts, turn(w[2 * width :]), tab)
    start = pl.multiple_of(domain * piece, piece)
    mine = parts[0][pl.ds(start, piece), :]
    rec = mm_nt(turn(w[width : 2 * width]), mine).astype(BF16)
    second = turn(w_out[2])
    agg[...] = jnp.zeros_like(agg)
    every = receivers[...]
    low = group * piece
    first_edge = jnp.sum((every < low).astype(jnp.int32))
    last_edge = jnp.sum((every < low + piece).astype(jnp.int32))

    def one(t, _):
        at = pl.multiple_of(t * tile, tile)
        block = edges[pl.ds(at, tile), :]
        side, spot = place(senders[:, pl.ds(at, tile)], owner_rows, piece, domains, group)
        row = side * (domains * piece) + spot
        both = mm_nt(mix, block)
        to = receivers[:, pl.ds(at, tile)] - low
        hot_to = hot(to, 0, small)
        first = both[:width] + mm(rec, hot_to)
        for c in range(tab.shape[0]):
            first += mm(tab[c], hot(row, c * CHUNK, blocks))
        y = mm(second, silu(first))
        new = (both[width:] + norm(y, 0)).astype(BF16)
        agg[...] += mm_nt(hot_to, new)
        return 0

    lax.fori_loop(first_edge // tile, (last_edge + tile - 1) // tile, one, 0)
    wn = w_node[1]
    first = mm(mine, wn[:width]) + mm(agg[...].astype(BF16), wn[width:])
    new = (mine.astype(F32) + mlp_rows(first, w_out[3])).astype(BF16)
    for s in range(domains):
        out[pl.ds(s * piece, piece), :] = new


def return_kernel(*refs, groups, owner_rows, piece, domains, nodes):
    parts = refs[:groups]
    packed, parents, w_node, w_out = refs[groups : groups + 4]
    out, coarse, tab = refs[groups + 4 :]
    group = lax.axis_index("grp")
    domain = lax.axis_index("dom")
    width = out.shape[1]
    blocks = steps(CHUNK)
    w = w_node[2]
    start = pl.multiple_of(domain * piece, piece)
    for side in range(groups):
        to = pl.multiple_of((group ^ side) * piece, piece)
        coarse[pl.ds(to, piece), :] = parts[side][pl.ds(start, piece), :]
    fill_table(parts, turn(w[width:]), tab)
    mine = packed[pl.ds(0, nodes), :]
    side, spot = place(parents[...], owner_rows, piece, domains, group)
    row = side * (domains * piece) + spot
    first = mm_nt(turn(w[:width]), mine)
    for c in range(tab.shape[0]):
        first += mm(tab[c], hot(row, c * CHUNK, blocks))
    y = norm(mm(turn(w_out[4]), silu(first)), 0)
    out[...] = (mine.astype(F32) + y.T).astype(BF16)


def spread(x, groups):
    held = {0: x}
    bit = groups >> 1
    while bit:
        for k in sorted(held):
            held[k | bit] = lax.ppermute(
                held[k], "grp", [(i, i ^ bit) for i in range(groups)]
            )
        bit >>= 1
    return [held[k] for k in range(groups)]


def swap(x):
    return lax.all_to_all(x, "dom", split_axis=0, concat_axis=0, tiled=True)


def per_device(
    fine_nodes,
    fine_edges,
    fine_senders,
    fine_receivers,
    edge_count,
    ghost_send,
    fine_parent,
    coarse_nodes,
    coarse_edges,
    coarse_senders,
    coarse_receivers,
    edge_in,
    node_in,
    mlp_out,
):
    domains = lax.axis_size("dom")
    groups = lax.axis_size("grp")
    local = fine_nodes[0]
    edges = fine_edges[0]
    nodes, width = local.shape
    slots = edges.shape[0]
    owner_rows = coarse_nodes.shape[0]
    coarse_slots = coarse_edges.shape[0]
    piece = owner_rows // groups
    ghosts = ghost_send.shape[1] * ghost_send.shape[2]
    sizes = dict(owner_rows=owner_rows, piece=piece, domains=domains)
    assert nodes % CHUNK == 0 and CHUNK % piece == 0 and piece <= LANES
    assert owner_rows * domains <= 1 << 14
    tile = max(t for t in (128, 256, 512, 1024) if slots % t == 0)
    ctile = max(t for t in (128, 256) if coarse_slots % t == 0)

    outgoing = pl.pallas_call(
        ghosts_kernel,
        out_shape=jax.ShapeDtypeStruct((ghosts, width), BF16),
        in_specs=[SMEM, VMEM],
        out_specs=VMEM,
        scratch_shapes=[pltpu.VMEM((nodes, width), F32), pltpu.VMEM((ghosts, width), F32)],
        name="ghosts",
    )(ghost_send[0], local)
    incoming = swap(outgoing)

    chunks = -(-(nodes + ghosts) // CHUNK)
    windows = nodes // CHUNK
    pack_rows = nodes + -(-2 * (nodes // LANES) // 16) * 16

    def whole(shape):
        return pl.BlockSpec(shape, lambda i: (0,) * len(shape))

    packed = pl.pallas_call(
        fine_kernel,
        out_shape=jax.ShapeDtypeStruct((pack_rows, width), BF16),
        grid=(slots // tile,),
        in_specs=[
            SMEM,
            pl.BlockSpec((1, tile), lambda i: (0, i), memory_space=pltpu.SMEM),
            pl.BlockSpec((tile, width), lambda i: (i, 0)),
            pl.BlockSpec((1, tile), lambda i: (0, i)),
            pl.BlockSpec((1, tile), lambda i: (0, i)),
            whole((nodes, width)),
            whole((ghosts, width)),
            whole((1, nodes)),
            pl.BlockSpec((None, 3 * width, width), lambda i: (0, 0, 0)),
            whole(node_in.shape),
            whole(mlp_out.shape),
        ],
        out_specs=whole((pack_rows, width)),
        scratch_shapes=[
            pltpu.VMEM((chunks, width, CHUNK), BF16),
            pltpu.VMEM((windows, width, CHUNK), BF16),
            pltpu.VMEM((width, tile), F32),
            pltpu.VMEM((nodes, width), F32),
            pltpu.VMEM((2 * width, width), BF16),
            pltpu.VMEM((width, width), BF16),
        ],
        name="fine",
    )(
        edge_count, fine_receivers, edges, fine_senders, fine_receivers, local, incoming,
        fine_parent, edge_in, node_in, mlp_out,
    )

    packs = spread(packed, groups)
    pooled = pl.pallas_call(
        functools.partial(pool_kernel, nodes=nodes, **sizes),
        out_shape=jax.ShapeDtypeStruct((domains * (piece + 16), width), BF16),
        in_specs=[VMEM] * groups,
        out_specs=VMEM,
        name="pool",
    )(*packs)
    got = swap(pooled)
    copies = jax.ShapeDtypeStruct((domains * piece, width), BF16)
    mid = pl.pallas_call(
        functools.partial(coarse_mid_kernel, piece=piece, domains=domains),
        out_shape=copies,
        in_specs=[VMEM] * 2,
        out_specs=VMEM,
        name="coarse_mid",
    )(got, coarse_nodes)
    table = pltpu.VMEM((owner_rows * domains // CHUNK, width, CHUNK), BF16)
    coarse = pl.pallas_call(
        functools.partial(coarse_kernel, groups=groups, tile=ctile, **sizes),
        out_shape=copies,
        in_specs=[VMEM] * (groups + 6),
        out_specs=VMEM,
        scratch_shapes=[table, pltpu.VMEM((piece, width), F32)],
        name="coarse",
    )(
        *spread(swap(mid), groups), coarse_edges, coarse_senders[None], coarse_receivers[None],
        edge_in, node_in, mlp_out,
    )
    fine_out, coarse_out = pl.pallas_call(
        functools.partial(return_kernel, groups=groups, nodes=nodes, **sizes),
        out_shape=(
            jax.ShapeDtypeStruct((nodes, width), BF16),
            jax.ShapeDtypeStruct((owner_rows, width), BF16),
        ),
        in_specs=[VMEM] * (groups + 4),
        out_specs=(VMEM, VMEM),
        scratch_shapes=[table],
        name="back",
    )(*spread(swap(coarse), groups), packed, fine_parent, node_in, mlp_out)
    return (fine_out[None], coarse_out)


def solution(mesh):
    placed = (
        P("grp", "dom", None),
        P("grp", "dom", None),
        P("grp", "dom"),
        P("grp", "dom"),
        P("grp", "dom"),
        P("grp", "dom", None),
        P("grp", "dom"),
        P("dom", None),
        P("dom", None),
        P("dom"),
        P("dom"),
        P(),
        P(),
        P(),
    )
    return jax.shard_map(
        per_device,
        mesh=mesh,
        in_specs=placed,
        out_specs=(P("grp", "dom", None), P("dom", None)),
        check_vma=False,
    )
```

```python
import functools

import jax
import jax.numpy as jnp
from jax import lax
from jax.experimental import pallas as pl
from jax.experimental.pallas import tpu as pltpu
from jax.sharding import PartitionSpec as P

F32 = jnp.float32
BF16 = jnp.bfloat16
NT = (((1,), (1,)), ((), ()))
CHUNK = 256
LANES = 128
VMEM = pl.BlockSpec(memory_space=pltpu.VMEM)
SMEM = pl.BlockSpec(memory_space=pltpu.SMEM)


def log2(n):
    bits = n.bit_length() - 1
    assert 1 << bits == n
    return bits


def mm(a, b):
    return jnp.dot(a, b, preferred_element_type=F32)


def mm_nt(a, b):
    return lax.dot_general(a, b, NT, preferred_element_type=F32)


def turn(w):
    return w.astype(F32).T.astype(BF16)


def silu(v):
    u = 0.5 * v
    return (u + u * jnp.tanh(u)).astype(BF16)


def norm(y, axis):
    centre = y - jnp.mean(y, axis, keepdims=True)
    spread = jnp.mean(centre * centre, axis, keepdims=True)
    return centre * lax.rsqrt(spread + 1e-05)


def mlp_rows(first, w_second):
    return norm(mm(silu(first), w_second), 1)


def steps(rows):
    base = lax.broadcasted_iota(jnp.int32, (16, LANES), 0)
    return [(base + 16 * j).astype(F32).astype(BF16) for j in range(rows // 16)]


def hot(row, base, blocks):
    rows = 16 * len(blocks)
    n = row.shape[1]
    near = jnp.clip(jnp.broadcast_to(row, (16, n)) - base, -1, rows).astype(F32).astype(BF16)
    one = jnp.ones((16, n), BF16)
    zero = jnp.zeros((16, n), BF16)
    return jnp.concatenate(
        [jnp.where(jnp.concatenate([b] * (n // LANES), 1) == near, one, zero) for b in blocks], 0
    )


def ghosts_kernel(send, local, out, wide, picked):
    wide[...] = local[...].astype(F32)
    peers, slots = send.shape

    def one(p, _):
        for k in range(slots):
            picked[pl.ds(p * slots + k, 1), :] = wide[pl.ds(send[p, k], 1), :]
        return 0

    lax.fori_loop(0, peers, one, 0)
    out[...] = picked[...].astype(BF16)


def windows_after(step, base, high):
    def run(k, _):
        step(base + LANES * k)
        return 0

    lax.fori_loop(1, (high - base) // LANES + 1, run, 0)


def chunk_list(rows):
    return [(c, min(CHUNK, rows - c)) for c in range(0, rows, CHUNK)]


def fine_first_kernel(
    count, bounds, edges, senders, receivers, local, w_edge, pre, turned, marks, rec, tab, w_self
):
    step = pl.program_id(0)
    tile = edges.shape[0]
    nodes, width = local.shape
    blocks = steps(CHUNK)
    small = steps(LANES)

    @pl.when(step == 0)
    def _():
        w = w_edge[...]
        w_send = turn(w[2 * width :])
        w_self[...] = turn(w[:width])
        mine = local[...]
        rec[...] = mm(mine, w[width : 2 * width]).astype(BF16)
        for c in range(tab.shape[0]):
            tab[c] = mm_nt(w_send, mine[c * CHUNK : (c + 1) * CHUNK]).astype(BF16)

    live = count[0, 0]
    at = step * tile

    @pl.when(at < live)
    def _():
        low = bounds[0, 0]
        high = bounds[0, jnp.minimum(tile, live - at) - 1]
        base = pl.multiple_of(jnp.minimum((low >> 4) << 4, nodes - LANES), 16)
        marks[0, step] = base
        marks[1, step] = high
        flat = edges[...].T
        turned[...] = flat
        slots = at + lax.broadcasted_iota(jnp.int32, (1, tile), 1)
        to = jnp.where(slots < live, receivers[...], -1)
        row = senders[...]
        first = mm(
            jnp.concatenate([w_self[...], rec[pl.ds(base, LANES), :].T], 1),
            jnp.concatenate([flat, hot(to, base, small)], 0),
        )
        for c in range(tab.shape[0]):
            first += mm(tab[c], hot(row, c * CHUNK, blocks))
        pre[...] = first

        def more(start):
            begin = pl.multiple_of(jnp.minimum(start, nodes - LANES), 16)
            far_to = jnp.where(to >= start, to, -1)
            pre[...] += mm(rec[pl.ds(begin, LANES), :].T, hot(far_to, begin, small))

        windows_after(more, base, high)


def fine_second_kernel(
    count, marks, pre, turned, senders, receivers, local, ghosts, parents, w_edge, w_node, w_out,
    out, agg, tabs, second,
):
    step = pl.program_id(0)
    width, tile = pre.shape
    nodes = local.shape[0]
    small = steps(LANES)
    blocks = steps(CHUNK)
    pieces = chunk_list(ghosts.shape[0])

    @pl.when(step == 0)
    def _():
        w_send = turn(w_edge[0][2 * width :])
        for j, (c, n) in enumerate(pieces):
            tabs[j, :, :n] = mm_nt(w_send, ghosts[pl.ds(c, n), :]).astype(BF16)
        second[...] = turn(w_out[0])
        agg[...] = jnp.zeros_like(agg)

    live = count[0, 0]
    at = step * tile

    @pl.when(at < live)
    def _():
        base = pl.multiple_of(marks[0, step], 16)
        high = marks[1, step]
        slots = at + lax.broadcasted_iota(jnp.int32, (1, tile), 1)
        to = jnp.where(slots < live, receivers[...], -1)
        row = senders[...]
        first = pre[...]
        for j, (c, n) in enumerate(pieces):
            first += mm(tabs[j, :, :n], hot(row, nodes + c, blocks[: n // 16]))
        y = mm(second[...], silu(first))
        new = (turned[...].astype(F32) + norm(y, 0)).astype(BF16)
        agg[pl.ds(base, LANES), :] += mm_nt(hot(to, base, small), new)

        def more(start):
            begin = pl.multiple_of(jnp.minimum(start, nodes - LANES), 16)
            far_to = jnp.where(to >= start, to, -1)
            agg[pl.ds(begin, LANES), :] += mm_nt(hot(far_to, begin, small), new)

        windows_after(more, base, high)

    @pl.when(step == pl.num_programs(0) - 1)
    def _():
        mine = local[...]
        w = w_node[0]
        first = mm(mine, w[:width]) + mm(agg[...].astype(BF16), w[width:])
        out[pl.ds(0, nodes), :] = (mine.astype(F32) + mlp_rows(first, w_out[1])).astype(BF16)
        ids = parents[...]
        lines = nodes // LANES
        pads = out.shape[0] - nodes - 2 * lines
        parts = [ids[:, j * LANES : (j + 1) * LANES] for j in range(lines)]
        digits = [p >> 6 for p in parts] + [p & 63 for p in parts]
        digits = digits + [jnp.zeros((1, LANES), jnp.int32)] * pads
        out[pl.ds(nodes, 2 * lines + pads), :] = (
            jnp.concatenate(digits, 0).astype(F32).astype(BF16)
        )


def place(ids, owner_rows, piece, domains, group):
    owner = ids >> log2(owner_rows)
    within = ids & (owner_rows - 1)
    return (within >> log2(piece)) ^ group, owner * piece + (within & (piece - 1))


def pool_kernel(*refs, owner_rows, piece, domains, nodes):
    packs, out = refs[:-1], refs[-1]
    group = lax.axis_index("grp")
    lines = nodes // LANES
    blocks = steps(CHUNK)
    width = out.shape[1]
    chunk_rows = piece + 16
    spots = []
    fulls = []
    for pack in packs:
        tail = pack[pl.ds(nodes, pack.shape[0] - nodes), :].astype(F32).astype(jnp.int32)
        ids = jnp.concatenate(
            [(tail[j : j + 1] << 6) + tail[lines + j : lines + j + 1] for j in range(lines)], 1
        )
        side, spot = place(ids, owner_rows, piece, domains, group)
        spots.append(jnp.where(side == 0, spot, -1))
        fulls.append(
            jnp.concatenate([pack[pl.ds(0, nodes), :], jnp.ones((nodes, LANES), BF16)], 1)
        )
    eye = lax.broadcasted_iota(jnp.int32, (piece, LANES), 0) == lax.broadcasted_iota(
        jnp.int32, (piece, LANES), 1
    )
    lane_row = lax.broadcasted_iota(jnp.int32, (16, LANES), 0)
    for c in range(domains * piece // CHUNK):
        total = mm(hot(spots[0], c * CHUNK, blocks), fulls[0])
        for spot, full in zip(spots[1:], fulls[1:]):
            total += mm(hot(spot, c * CHUNK, blocks), full)
        for q in range(CHUNK // piece):
            base = (c * CHUNK // piece + q) * chunk_rows
            part = total[q * piece : (q + 1) * piece]
            out[pl.ds(base, piece), :] = part[:, :width].astype(BF16)
            many = jnp.sum(jnp.where(eye, part[:, width:], 0.0), 0, keepdims=True)
            high = jnp.floor(many * (1.0 / 256.0))
            low = many - 256.0 * high
            both = jnp.where(lane_row == 0, high, jnp.where(lane_row == 1, low, 0.0))
            out[pl.ds(base + piece, 16), :] = both.astype(BF16)


def coarse_mid_kernel(got, nodes, out, *, piece, domains):
    group = lax.axis_index("grp")
    chunk_rows = piece + 16
    parts = [got[pl.ds(s * chunk_rows, chunk_rows), :].astype(F32) for s in range(domains)]
    total = functools.reduce(jnp.add, parts)
    row = 256.0 * total[piece : piece + 1] + total[piece + 1 : piece + 2]
    eye = lax.broadcasted_iota(jnp.int32, (piece, LANES), 0) == lax.broadcasted_iota(
        jnp.int32, (piece, LANES), 1
    )
    many = jnp.sum(jnp.where(eye, jnp.broadcast_to(row, (piece, LANES)), 0.0), 1, keepdims=True)
    start = pl.multiple_of(group * piece, piece)
    mine = nodes[pl.ds(start, piece), :].astype(F32)
    mid = ((mine + total[:piece]) / (1.0 + many)).astype(BF16)
    for s in range(domains):
        out[pl.ds(s * piece, piece), :] = mid


def fill_table(parts, w, tab):
    per = parts[0].shape[0] // CHUNK
    for k, part in enumerate(parts):
        for c in range(per):
            tab[k * per + c] = mm_nt(w, part[pl.ds(c * CHUNK, CHUNK), :]).astype(BF16)


def coarse_kernel(
    *refs, groups, owner_rows, piece, domains, tile
):
    parts = refs[:groups]
    edges, senders, receivers, w_edge, w_node, w_out = refs[groups : groups + 6]
    out, tab, agg = refs[groups + 6 :]
    group = lax.axis_index("grp")
    domain = lax.axis_index("dom")
    width = edges.shape[1]
    blocks = steps(CHUNK)
    small = steps(piece)
    w = w_edge[1]
    fill_table(parts, turn(w[2 * width :]), tab)
    start = pl.multiple_of(domain * piece, piece)
    mine = parts[0][pl.ds(start, piece), :]
    rec = mm_nt(turn(w[width : 2 * width]), mine).astype(BF16)
    mix = jnp.concatenate([turn(w[:width]), rec], 1)
    second = turn(w_out[2])
    agg[...] = jnp.zeros_like(agg)
    every = receivers[...]
    low = group * piece
    first_edge = jnp.sum((every < low).astype(jnp.int32))
    last_edge = jnp.sum((every < low + piece).astype(jnp.int32))

    begin = (first_edge >> log2(LANES)) << log2(LANES)

    def one(t, _):
        wanted = begin + t * tile
        at = pl.multiple_of(jnp.minimum(wanted, edges.shape[0] - tile), LANES)
        here = pl.ds(at, tile)
        side, spot = place(senders[:, here], owner_rows, piece, domains, group)
        row = side * (domains * piece) + spot
        flat = edges[here, :].T
        slots = at + lax.broadcasted_iota(jnp.int32, (1, tile), 1)
        to = jnp.where(slots >= wanted, receivers[:, here] - low, -1)
        hot_to = hot(to, 0, small)
        first = mm(mix, jnp.concatenate([flat, hot_to], 0))
        for c in range(tab.shape[0]):
            first += mm(tab[c], hot(row, c * CHUNK, blocks))
        y = mm(second, silu(first))
        new = (flat.astype(F32) + norm(y, 0)).astype(BF16)
        agg[...] += mm_nt(hot_to, new)
        return 0

    lax.fori_loop(0, (last_edge - begin + tile - 1) // tile, one, 0)
    wn = w_node[1]
    first = mm(mine, wn[:width]) + mm(agg[...].astype(BF16), wn[width:])
    new = (mine.astype(F32) + mlp_rows(first, w_out[3])).astype(BF16)
    for s in range(domains):
        out[pl.ds(s * piece, piece), :] = new


def return_kernel(*refs, groups, owner_rows, piece, domains, nodes):
    parts = refs[:groups]
    packed, parents, w_node, w_out = refs[groups : groups + 4]
    out, coarse, tab = refs[groups + 4 :]
    group = lax.axis_index("grp")
    domain = lax.axis_index("dom")
    width = out.shape[1]
    blocks = steps(CHUNK)
    w = w_node[2]
    start = pl.multiple_of(domain * piece, piece)
    for side in range(groups):
        to = pl.multiple_of((group ^ side) * piece, piece)
        coarse[pl.ds(to, piece), :] = parts[side][pl.ds(start, piece), :]
    fill_table(parts, turn(w[width:]), tab)
    mine = packed[pl.ds(0, nodes), :]
    side, spot = place(parents[...], owner_rows, piece, domains, group)
    row = side * (domains * piece) + spot
    first = mm_nt(turn(w[:width]), mine)
    for c in range(tab.shape[0]):
        first += mm(tab[c], hot(row, c * CHUNK, blocks))
    y = norm(mm(turn(w_out[4]), silu(first)), 0)
    out[...] = (mine.astype(F32) + y.T).astype(BF16)


def spread(x, groups):
    held = {0: x}
    bit = groups >> 1
    while bit:
        for k in sorted(held):
            held[k | bit] = lax.ppermute(
                held[k], "grp", [(i, i ^ bit) for i in range(groups)]
            )
        bit >>= 1
    return [held[k] for k in range(groups)]


def near(x):
    return pltpu.with_memory_space_constraint(x, pltpu.VMEM)


def far(x):
    return pltpu.with_memory_space_constraint(x, pltpu.HBM)


def swap(x):
    return lax.all_to_all(x, "dom", split_axis=0, concat_axis=0, tiled=True)


def per_device(
    fine_nodes,
    fine_edges,
    fine_senders,
    fine_receivers,
    edge_count,
    ghost_send,
    fine_parent,
    coarse_nodes,
    coarse_edges,
    coarse_senders,
    coarse_receivers,
    edge_in,
    node_in,
    mlp_out,
):
    domains = lax.axis_size("dom")
    groups = lax.axis_size("grp")
    local = fine_nodes[0]
    edges = fine_edges[0]
    nodes, width = local.shape
    slots = edges.shape[0]
    owner_rows = coarse_nodes.shape[0]
    coarse_slots = coarse_edges.shape[0]
    piece = owner_rows // groups
    ghosts = ghost_send.shape[1] * ghost_send.shape[2]
    sizes = dict(owner_rows=owner_rows, piece=piece, domains=domains)
    assert nodes % CHUNK == 0 and CHUNK % piece == 0 and piece <= LANES
    assert owner_rows * domains <= 1 << 14
    tile = max(t for t in (128, 256, 512, 768, 1536) if slots % t == 0)
    ctile = max(t for t in (128, 256) if coarse_slots % t == 0)

    params = pltpu.CompilerParams(vmem_limit_bytes=24 << 20)
    w_edge = near(edge_in)
    w_node = near(node_in)
    w_out = near(mlp_out)
    parents = near(fine_parent)

    outgoing = pl.pallas_call(
        ghosts_kernel,
        out_shape=pltpu.VMEM((ghosts, width), BF16),
        in_specs=[SMEM, VMEM],
        out_specs=VMEM,
        scratch_shapes=[pltpu.VMEM((nodes, width), F32), pltpu.VMEM((ghosts, width), F32)],
        compiler_params=params,
        name="ghosts",
    )(far(ghost_send[0]), far(local))
    incoming = near(swap(outgoing))

    tiles = slots // tile
    row_tile = pl.BlockSpec((1, tile), lambda i: (0, i))
    square = pl.BlockSpec((None, width, tile), lambda i: (i, 0, 0))

    def whole(shape):
        return pl.BlockSpec(shape, lambda i: (0,) * len(shape))

    pre, turned, marks = pl.pallas_call(
        fine_first_kernel,
        grid=(tiles,),
        out_shape=(
            pltpu.HBM((tiles, width, tile), F32),
            pltpu.HBM((tiles, width, tile), BF16),
            jax.ShapeDtypeStruct((2, tiles), jnp.int32),
        ),
        in_specs=[
            SMEM,
            pl.BlockSpec((1, tile), lambda i: (0, i), memory_space=pltpu.SMEM),
            pl.BlockSpec((tile, width), lambda i: (i, 0)),
            row_tile,
            row_tile,
            whole((nodes, width)),
            pl.BlockSpec((None, 3 * width, width), lambda i: (0, 0, 0)),
        ],
        out_specs=(square, square, SMEM),
        scratch_shapes=[
            pltpu.VMEM((nodes, width), BF16),
            pltpu.VMEM((nodes // CHUNK, width, CHUNK), BF16),
            pltpu.VMEM((width, width), BF16),
        ],
        compiler_params=params,
        cost_estimate=pl.CostEstimate(
            flops=2 * slots * width * (nodes + 2 * width), transcendentals=0, bytes_accessed=0
        ),
        name="fine_first",
    )(
        edge_count, far(fine_receivers), far(edges), far(fine_senders), far(fine_receivers),
        far(local), far(edge_in),
    )

    pack_rows = nodes + -(-2 * (nodes // LANES) // 16) * 16
    packed = pl.pallas_call(
        fine_second_kernel,
        grid=(tiles,),
        out_shape=pltpu.VMEM((pack_rows, width), BF16),
        in_specs=[SMEM, SMEM, square, square, row_tile, row_tile] + [VMEM] * 6,
        out_specs=VMEM,
        scratch_shapes=[
            pltpu.VMEM((nodes, width), F32),
            pltpu.VMEM((len(chunk_list(ghosts)), width, CHUNK), BF16),
            pltpu.VMEM((width, width), BF16),
        ],
        compiler_params=params,
        name="fine_second",
    )(
        edge_count, marks, far(pre), far(turned), far(fine_senders), far(fine_receivers),
        near(local), incoming, parents, w_edge, w_node, w_out,
    )
    packed = near(packed)

    packs = [near(p) for p in spread(packed, groups)]
    pooled = pl.pallas_call(
        functools.partial(pool_kernel, nodes=nodes, **sizes),
        out_shape=pltpu.VMEM((domains * (piece + 16), width), BF16),
        in_specs=[VMEM] * groups,
        out_specs=VMEM,
        compiler_params=params,
        name="pool",
    )(*packs)
    got = near(swap(pooled))
    copies = pltpu.VMEM((domains * piece, width), BF16)
    mid = pl.pallas_call(
        functools.partial(coarse_mid_kernel, piece=piece, domains=domains),
        out_shape=copies,
        in_specs=[VMEM] * 2,
        out_specs=VMEM,
        compiler_params=params,
        name="coarse_mid",
    )(got, near(coarse_nodes))
    table = pltpu.VMEM((owner_rows * domains // CHUNK, width, CHUNK), BF16)
    coarse = pl.pallas_call(
        functools.partial(coarse_kernel, groups=groups, tile=ctile, **sizes),
        out_shape=copies,
        in_specs=[VMEM] * (groups + 6),
        out_specs=VMEM,
        scratch_shapes=[table, pltpu.VMEM((piece, width), F32)],
        compiler_params=params,
        name="coarse",
    )(
        *[near(p) for p in spread(swap(mid), groups)], near(coarse_edges),
        near(coarse_senders[None]), near(coarse_receivers[None]), w_edge, w_node, w_out,
    )
    fine_out, coarse_out = pl.pallas_call(
        functools.partial(return_kernel, groups=groups, nodes=nodes, **sizes),
        out_shape=(
            jax.ShapeDtypeStruct((nodes, width), BF16),
            jax.ShapeDtypeStruct((owner_rows, width), BF16),
        ),
        in_specs=[VMEM] * (groups + 4),
        out_specs=(VMEM, VMEM),
        scratch_shapes=[table],
        compiler_params=params,
        name="back",
    )(*[near(p) for p in spread(swap(coarse), groups)], packed, parents, w_node, w_out)
    return (fine_out[None], coarse_out)


def solution(mesh):
    placed = (
        P("grp", "dom", None),
        P("grp", "dom", None),
        P("grp", "dom"),
        P("grp", "dom"),
        P("grp", "dom"),
        P("grp", "dom", None),
        P("grp", "dom"),
        P("dom", None),
        P("dom", None),
        P("dom"),
        P("dom"),
        P(),
        P(),
        P(),
    )
    return jax.shard_map(
        per_device,
        mesh=mesh,
        in_specs=placed,
        out_specs=(P("grp", "dom", None), P("dom", None)),
        check_vma=False,
    )
```

```python
import functools

import jax
import jax.numpy as jnp
from jax import lax
from jax.experimental import pallas as pl
from jax.experimental.pallas import tpu as pltpu
from jax.sharding import PartitionSpec as P

F32 = jnp.float32
BF16 = jnp.bfloat16
NT = (((1,), (1,)), ((), ()))
CHUNK = 256
SUB = 256
SUB2 = 256
LANES = 128
VMEM = pl.BlockSpec(memory_space=pltpu.VMEM)
SMEM = pl.BlockSpec(memory_space=pltpu.SMEM)


def log2(n):
    bits = n.bit_length() - 1
    assert 1 << bits == n
    return bits


def mm(a, b):
    return jnp.dot(a, b, preferred_element_type=F32)


def mm_nt(a, b):
    return lax.dot_general(a, b, NT, preferred_element_type=F32)


def turn(w):
    return w.astype(F32).T.astype(BF16)


def silu(v):
    u = 0.5 * v
    return (u + u * jnp.tanh(u)).astype(BF16)


def norm(y, axis):
    centre = y - jnp.mean(y, axis, keepdims=True)
    spread = jnp.mean(centre * centre, axis, keepdims=True)
    return centre * lax.rsqrt(spread + 1e-05)


def mlp_rows(first, w_second):
    return norm(mm(silu(first), w_second), 1)


def steps(rows):
    base = lax.broadcasted_iota(jnp.int32, (16, LANES), 0)
    return [(base + 16 * j).astype(F32).astype(BF16) for j in range(rows // 16)]


def hot(row, base, blocks):
    rows = 16 * len(blocks)
    n = row.shape[1]
    near = jnp.clip(jnp.broadcast_to(row, (16, n)) - base, -1, rows).astype(F32).astype(BF16)
    one = jnp.ones((16, n), BF16)
    zero = jnp.zeros((16, n), BF16)
    return jnp.concatenate(
        [jnp.where(jnp.concatenate([b] * (n // LANES), 1) == near, one, zero) for b in blocks], 0
    )


def ghosts_kernel(send, local, out, wide, picked):
    wide[...] = local[...].astype(F32)
    peers, slots = send.shape

    def one(p, _):
        for k in range(slots):
            picked[pl.ds(p * slots + k, 1), :] = wide[pl.ds(send[p, k], 1), :]
        return 0

    lax.fori_loop(0, peers, one, 0)
    out[...] = picked[...].astype(BF16)


def windows_after(step, base, high, rows):
    def run(k, _):
        step(base + rows * k)
        return 0

    lax.fori_loop(1, (high - base) // rows + 1, run, 0)


def chunk_list(rows):
    return [(c, min(CHUNK, rows - c)) for c in range(0, rows, CHUNK)]


def fine_first_kernel(
    count, bounds, edges, senders, receivers, local, w_edge, pre, agg, marks, rec, *, span
):
    nodes, width = local.shape
    tile = pre.shape[2]
    blocks = steps(CHUNK)
    small = steps(LANES)
    w = w_edge[0]
    w_send = turn(w[2 * width :])
    mine = local[...]
    rec[...] = mm(mine, w[width : 2 * width]).astype(BF16)
    tabs = [
        mm_nt(w_send, mine[c : c + CHUNK]).astype(BF16) for c in range(0, nodes, CHUNK)
    ]
    fixed = jnp.concatenate([turn(w[:width])] + tabs, 1)
    agg[...] = jnp.zeros_like(agg)
    live = count[0, 0]

    def one(t, _):
        later = []
        for p in range(0, tile, span):
            at = pl.multiple_of(t * tile + p, span)
            low = bounds[0, at]
            high = bounds[0, jnp.minimum(at + span, live) - 1]
            base = pl.multiple_of(jnp.minimum((low >> 4) << 4, nodes - LANES), 16)
            marks[0, t * (tile // span) + p // span] = base
            marks[1, t * (tile // span) + p // span] = high
            slots = at + lax.broadcasted_iota(jnp.int32, (1, span), 1)
            to = jnp.where(slots < live, receivers[:, pl.ds(at, span)], -1)
            left = jnp.concatenate([fixed, rec[pl.ds(base, LANES), :].T], 1)
            hots = []
            for n in range(0, span, SUB):
                row = senders[:, pl.ds(at + n, SUB)]
                hot_to = hot(to[:, n : n + SUB], base, small)
                right = [edges[pl.ds(at + n, SUB), :].T]
                right += [hot(row, c, blocks) for c in range(0, nodes, CHUNK)]
                full = mm(left, jnp.concatenate(right + [hot_to], 0))
                pre[t, :, p + n : p + n + SUB] = full.astype(BF16)
                hots.append(hot_to)
            agg[pl.ds(base, LANES), :] += mm(jnp.concatenate(hots, 1), edges[pl.ds(at, span), :])

            def more(start, at=at, to=to, p=p):
                begin = pl.multiple_of(jnp.minimum(start, nodes - LANES), 16)
                hot_far = hot(jnp.where(to >= start, to, -1), begin, small)
                extra = mm(rec[pl.ds(begin, LANES), :].T, hot_far)
                here = pre[t, :, p : p + span].astype(F32)
                pre[t, :, p : p + span] = (here + extra).astype(BF16)
                agg[pl.ds(begin, LANES), :] += mm(hot_far, edges[pl.ds(at, span), :])

            later.append((more, base, high, LANES))
        for item in later:
            windows_after(*item)
        return 0

    lax.fori_loop(0, (live + tile - 1) // tile, one, 0)


def fine_second_kernel(
    count, marks, pre, some, senders, receivers, local, ghosts, parents, w_edge, w_node, w_out,
    out, agg, *, span,
):
    tile = pre.shape[2]
    nodes, width = local.shape
    wide = 2 * span if tile % (2 * span) == 0 else span
    blocks = steps(CHUNK)
    pieces = chunk_list(ghosts.shape[0])
    w_send = turn(w_edge[0][2 * width :])
    tabs = [mm_nt(w_send, ghosts[pl.ds(c, n), :]).astype(BF16) for c, n in pieces]
    second = turn(w_out[0])
    agg[...] = some[...]
    live = count[0, 0]

    def one(t, _):
        later = []
        for p in range(0, tile, wide):
            at = pl.multiple_of(t * tile + p, wide)
            mark = t * (tile // span) + p // span
            base = pl.multiple_of(jnp.minimum(marks[0, mark], nodes - CHUNK), 16)
            high = marks[1, mark + wide // span - 1]
            slots = at + lax.broadcasted_iota(jnp.int32, (1, wide), 1)
            to = jnp.where(slots < live, receivers[:, pl.ds(at, wide)], -1)
            news = []
            for n in range(0, wide, SUB2):
                row = senders[:, pl.ds(at + n, SUB2)]
                first = pre[t, :, p + n : p + n + SUB2].astype(F32)
                for (c, k), tab in zip(pieces, tabs):
                    first += mm(tab, hot(row, nodes + c, blocks[: k // 16]))
                news.append(norm(mm(second, silu(first)), 0).astype(BF16))
            new = jnp.concatenate(news, 1)
            agg[pl.ds(base, CHUNK), :] += mm_nt(hot(to, base, blocks), new)

            def more(start, to=to, new=new):
                begin = pl.multiple_of(jnp.minimum(start, nodes - CHUNK), 16)
                far_to = jnp.where(to >= start, to, -1)
                agg[pl.ds(begin, CHUNK), :] += mm_nt(hot(far_to, begin, blocks), new)

            later.append((more, base, high, CHUNK))
        for item in later:
            windows_after(*item)
        return 0

    lax.fori_loop(0, (live + tile - 1) // tile, one, 0)
    mine = local[...]
    w = w_node[0]
    first = mm(mine, w[:width]) + mm(agg[...].astype(BF16), w[width:])
    out[pl.ds(0, nodes), :] = (mine.astype(F32) + mlp_rows(first, w_out[1])).astype(BF16)
    ids = parents[...]
    lines = nodes // LANES
    pads = out.shape[0] - nodes - 2 * lines
    parts = [ids[:, j * LANES : (j + 1) * LANES] for j in range(lines)]
    digits = [p >> 6 for p in parts] + [p & 63 for p in parts]
    digits = digits + [jnp.zeros((1, LANES), jnp.int32)] * pads
    out[pl.ds(nodes, 2 * lines + pads), :] = jnp.concatenate(digits, 0).astype(F32).astype(BF16)


def place(ids, owner_rows, piece, domains, group):
    owner = ids >> log2(owner_rows)
    within = ids & (owner_rows - 1)
    return (within >> log2(piece)) ^ group, owner * piece + (within & (piece - 1))


def pool_kernel(*refs, owner_rows, piece, domains, nodes):
    packs, out = refs[:-1], refs[-1]
    group = lax.axis_index("grp")
    lines = nodes // LANES
    blocks = steps(CHUNK)
    width = out.shape[1]
    chunk_rows = piece + 16
    spots = []
    fulls = []
    for pack in packs:
        tail = pack[pl.ds(nodes, pack.shape[0] - nodes), :].astype(F32).astype(jnp.int32)
        ids = jnp.concatenate(
            [(tail[j : j + 1] << 6) + tail[lines + j : lines + j + 1] for j in range(lines)], 1
        )
        side, spot = place(ids, owner_rows, piece, domains, group)
        spots.append(jnp.where(side == 0, spot, -1))
        fulls.append(
            jnp.concatenate([pack[pl.ds(0, nodes), :], jnp.ones((nodes, LANES), BF16)], 1)
        )
    eye = lax.broadcasted_iota(jnp.int32, (piece, LANES), 0) == lax.broadcasted_iota(
        jnp.int32, (piece, LANES), 1
    )
    lane_row = lax.broadcasted_iota(jnp.int32, (16, LANES), 0)
    for c in range(domains * piece // CHUNK):
        total = mm(hot(spots[0], c * CHUNK, blocks), fulls[0])
        for spot, full in zip(spots[1:], fulls[1:]):
            total += mm(hot(spot, c * CHUNK, blocks), full)
        for q in range(CHUNK // piece):
            base = (c * CHUNK // piece + q) * chunk_rows
            part = total[q * piece : (q + 1) * piece]
            out[pl.ds(base, piece), :] = part[:, :width].astype(BF16)
            many = jnp.sum(jnp.where(eye, part[:, width:], 0.0), 0, keepdims=True)
            high = jnp.floor(many * (1.0 / 256.0))
            low = many - 256.0 * high
            both = jnp.where(lane_row == 0, high, jnp.where(lane_row == 1, low, 0.0))
            out[pl.ds(base + piece, 16), :] = both.astype(BF16)


def coarse_mid_kernel(got, nodes, out, *, piece, domains):
    group = lax.axis_index("grp")
    chunk_rows = piece + 16
    parts = [got[pl.ds(s * chunk_rows, chunk_rows), :].astype(F32) for s in range(domains)]
    total = functools.reduce(jnp.add, parts)
    row = 256.0 * total[piece : piece + 1] + total[piece + 1 : piece + 2]
    eye = lax.broadcasted_iota(jnp.int32, (piece, LANES), 0) == lax.broadcasted_iota(
        jnp.int32, (piece, LANES), 1
    )
    many = jnp.sum(jnp.where(eye, jnp.broadcast_to(row, (piece, LANES)), 0.0), 1, keepdims=True)
    start = pl.multiple_of(group * piece, piece)
    mine = nodes[pl.ds(start, piece), :].astype(F32)
    mid = ((mine + total[:piece]) / (1.0 + many)).astype(BF16)
    for s in range(domains):
        out[pl.ds(s * piece, piece), :] = mid


def fill_table(parts, w, tab):
    per = parts[0].shape[0] // CHUNK
    for k, part in enumerate(parts):
        for c in range(per):
            tab[k * per + c] = mm_nt(w, part[pl.ds(c * CHUNK, CHUNK), :]).astype(BF16)


def look(tab, row, blocks):
    total = 0.0
    for c in range(0, tab.shape[0], 4):
        left = jnp.concatenate([tab[c + j] for j in range(4)], 1)
        total += mm(left, jnp.concatenate([hot(row, (c + j) * CHUNK, blocks) for j in range(4)], 0))
    return total


def coarse_kernel(
    *refs, groups, owner_rows, piece, domains, tile
):
    parts = refs[:groups]
    edges, senders, receivers, w_edge, w_node, w_out = refs[groups : groups + 6]
    out, tab, agg = refs[groups + 6 :]
    group = lax.axis_index("grp")
    domain = lax.axis_index("dom")
    width = edges.shape[1]
    blocks = steps(CHUNK)
    small = steps(piece)
    w = w_edge[1]
    fill_table(parts, turn(w[2 * width :]), tab)
    start = pl.multiple_of(domain * piece, piece)
    mine = parts[0][pl.ds(start, piece), :]
    rec = mm_nt(turn(w[width : 2 * width]), mine).astype(BF16)
    mix = jnp.concatenate([turn(w[:width]), rec], 1)
    second = turn(w_out[2])
    agg[...] = jnp.zeros_like(agg)
    every = receivers[...]
    low = group * piece
    first_edge = jnp.sum((every < low).astype(jnp.int32))
    last_edge = jnp.sum((every < low + piece).astype(jnp.int32))

    begin = (first_edge >> log2(LANES)) << log2(LANES)

    def one(t, _):
        wanted = begin + t * tile
        at = pl.multiple_of(jnp.minimum(wanted, edges.shape[0] - tile), LANES)
        here = pl.ds(at, tile)
        side, spot = place(senders[:, here], owner_rows, piece, domains, group)
        row = side * (domains * piece) + spot
        flat = edges[here, :].T
        slots = at + lax.broadcasted_iota(jnp.int32, (1, tile), 1)
        to = jnp.where(slots >= wanted, receivers[:, here] - low, -1)
        hot_to = hot(to, 0, small)
        first = mm(mix, jnp.concatenate([flat, hot_to], 0)) + look(tab, row, blocks)
        y = mm(second, silu(first))
        new = (flat.astype(F32) + norm(y, 0)).astype(BF16)
        agg[...] += mm_nt(hot_to, new)
        return 0

    lax.fori_loop(0, (last_edge - begin + tile - 1) // tile, one, 0)
    wn = w_node[1]
    first = mm(mine, wn[:width]) + mm(agg[...].astype(BF16), wn[width:])
    new = (mine.astype(F32) + mlp_rows(first, w_out[3])).astype(BF16)
    for s in range(domains):
        out[pl.ds(s * piece, piece), :] = new


def return_kernel(*refs, groups, owner_rows, piece, domains, nodes):
    parts = refs[:groups]
    packed, parents, w_node, w_out = refs[groups : groups + 4]
    out, coarse, tab = refs[groups + 4 :]
    group = lax.axis_index("grp")
    domain = lax.axis_index("dom")
    width = out.shape[1]
    blocks = steps(CHUNK)
    w = w_node[2]
    start = pl.multiple_of(domain * piece, piece)
    for side in range(groups):
        to = pl.multiple_of((group ^ side) * piece, piece)
        coarse[pl.ds(to, piece), :] = parts[side][pl.ds(start, piece), :]
    fill_table(parts, turn(w[width:]), tab)
    side, spot = place(parents[...], owner_rows, piece, domains, group)
    row = side * (domains * piece) + spot
    mine = packed[pl.ds(0, nodes), :]
    first = mm_nt(turn(w[:width]), mine)
    for c in range(tab.shape[0]):
        first += mm(tab[c], hot(row, c * CHUNK, blocks))
    y = norm(mm(turn(w_out[4]), silu(first)), 0)
    out[...] = (mine.astype(F32) + y.T).astype(BF16)


def spread(x, groups):
    held = {0: x}
    bit = groups >> 1
    while bit:
        for k in sorted(held):
            held[k | bit] = lax.ppermute(
                held[k], "grp", [(i, i ^ bit) for i in range(groups)]
            )
        bit >>= 1
    return [held[k] for k in range(groups)]


def near(x):
    return pltpu.with_memory_space_constraint(x, pltpu.VMEM)


def far(x):
    return pltpu.with_memory_space_constraint(x, pltpu.HBM)


def swap(x):
    return lax.all_to_all(x, "dom", split_axis=0, concat_axis=0, tiled=True)


def per_device(
    fine_nodes,
    fine_edges,
    fine_senders,
    fine_receivers,
    edge_count,
    ghost_send,
    fine_parent,
    coarse_nodes,
    coarse_edges,
    coarse_senders,
    coarse_receivers,
    edge_in,
    node_in,
    mlp_out,
):
    domains = lax.axis_size("dom")
    groups = lax.axis_size("grp")
    local = fine_nodes[0]
    edges = fine_edges[0]
    nodes, width = local.shape
    slots = edges.shape[0]
    owner_rows = coarse_nodes.shape[0]
    coarse_slots = coarse_edges.shape[0]
    piece = owner_rows // groups
    ghosts = ghost_send.shape[1] * ghost_send.shape[2]
    sizes = dict(owner_rows=owner_rows, piece=piece, domains=domains)
    assert nodes % CHUNK == 0 and CHUNK % piece == 0 and piece <= LANES
    assert owner_rows * domains <= 1 << 14
    span = max(t for t in (256, 512, 768) if slots % t == 0)
    tile = max(span * k for k in (1, 2, 4) if slots % (span * k) == 0)
    ctile = max(t for t in (128, 256) if coarse_slots % t == 0)

    params = pltpu.CompilerParams(vmem_limit_bytes=24 << 20)
    w_edge = near(edge_in)
    w_node = near(node_in)
    w_out = near(mlp_out)
    parents = near(fine_parent)

    outgoing = pl.pallas_call(
        ghosts_kernel,
        out_shape=pltpu.VMEM((ghosts, width), BF16),
        in_specs=[SMEM, VMEM],
        out_specs=VMEM,
        scratch_shapes=[pltpu.VMEM((nodes, width), F32), pltpu.VMEM((ghosts, width), F32)],
        compiler_params=params,
        name="ghosts",
    )(far(ghost_send[0]), far(local))
    incoming = near(swap(outgoing))

    tiles = slots // tile
    pre, some, marks = pl.pallas_call(
        functools.partial(fine_first_kernel, span=span),
        out_shape=(
            pltpu.VMEM((tiles, width, tile), BF16),
            pltpu.VMEM((nodes, width), F32),
            pltpu.HBM((2, slots // span), jnp.int32),
        ),
        in_specs=[SMEM, SMEM] + [VMEM] * 5,
        out_specs=(VMEM, VMEM, SMEM),
        scratch_shapes=[pltpu.VMEM((nodes, width), BF16)],
        compiler_params=params,
        cost_estimate=pl.CostEstimate(
            flops=2 * slots * width * (nodes + 2 * width), transcendentals=0, bytes_accessed=0
        ),
        name="fine_first",
    )(
        edge_count, far(fine_receivers), far(edges), far(fine_senders), far(fine_receivers),
        far(local), far(edge_in),
    )

    pack_rows = nodes + -(-2 * (nodes // LANES) // 16) * 16
    packed = pl.pallas_call(
        functools.partial(fine_second_kernel, span=span),
        out_shape=pltpu.VMEM((pack_rows, width), BF16),
        in_specs=[SMEM, SMEM] + [VMEM] * 10,
        out_specs=VMEM,
        scratch_shapes=[pltpu.VMEM((nodes, width), F32)],
        compiler_params=params,
        name="fine_second",
    )(
        edge_count, far(marks), near(pre), near(some), far(fine_senders), far(fine_receivers),
        near(local), incoming, far(fine_parent), w_edge, w_node, w_out,
    )
    packed = near(packed)

    packs = [near(p) for p in spread(packed, groups)]
    pooled = pl.pallas_call(
        functools.partial(pool_kernel, nodes=nodes, **sizes),
        out_shape=pltpu.VMEM((domains * (piece + 16), width), BF16),
        in_specs=[VMEM] * groups,
        out_specs=VMEM,
        compiler_params=params,
        name="pool",
    )(*packs)
    got = near(swap(pooled))
    copies = pltpu.VMEM((domains * piece, width), BF16)
    mid = pl.pallas_call(
        functools.partial(coarse_mid_kernel, piece=piece, domains=domains),
        out_shape=copies,
        in_specs=[VMEM] * 2,
        out_specs=VMEM,
        compiler_params=params,
        name="coarse_mid",
    )(got, near(coarse_nodes))
    table = pltpu.VMEM((owner_rows * domains // CHUNK, width, CHUNK), BF16)
    coarse = pl.pallas_call(
        functools.partial(coarse_kernel, groups=groups, tile=ctile, **sizes),
        out_shape=copies,
        in_specs=[VMEM] * (groups + 6),
        out_specs=VMEM,
        scratch_shapes=[table, pltpu.VMEM((piece, width), F32)],
        compiler_params=params,
        name="coarse",
    )(
        *[near(p) for p in spread(swap(mid), groups)], near(coarse_edges),
        near(coarse_senders[None]), near(coarse_receivers[None]), w_edge, w_node, w_out,
    )
    fine_out, coarse_out = pl.pallas_call(
        functools.partial(return_kernel, groups=groups, nodes=nodes, **sizes),
        out_shape=(
            jax.ShapeDtypeStruct((nodes, width), BF16),
            jax.ShapeDtypeStruct((owner_rows, width), BF16),
        ),
        in_specs=[VMEM] * (groups + 4),
        out_specs=(VMEM, VMEM),
        scratch_shapes=[table],
        compiler_params=params,
        name="back",
    )(*[near(p) for p in spread(swap(coarse), groups)], packed, parents, w_node, w_out)
    return (fine_out[None], coarse_out)


def solution(mesh):
    placed = (
        P("grp", "dom", None),
        P("grp", "dom", None),
        P("grp", "dom"),
        P("grp", "dom"),
        P("grp", "dom"),
        P("grp", "dom", None),
        P("grp", "dom"),
        P("dom", None),
        P("dom", None),
        P("dom"),
        P("dom"),
        P(),
        P(),
        P(),
    )
    return jax.shard_map(
        per_device,
        mesh=mesh,
        in_specs=placed,
        out_specs=(P("grp", "dom", None), P("dom", None)),
        check_vma=False,
    )
```

```python
import functools

import jax
import jax.numpy as jnp
from jax import lax
from jax.experimental import pallas as pl
from jax.experimental.pallas import tpu as pltpu
from jax.sharding import PartitionSpec as P

F32 = jnp.float32
BF16 = jnp.bfloat16
NT = (((1,), (1,)), ((), ()))
CHUNK = 256
SUB = 256
SUB2 = 256
LANES = 128
VMEM = pl.BlockSpec(memory_space=pltpu.VMEM)
SMEM = pl.BlockSpec(memory_space=pltpu.SMEM)


def log2(n):
    bits = n.bit_length() - 1
    assert 1 << bits == n
    return bits


def mm(a, b):
    return jnp.dot(a, b, preferred_element_type=F32)


def mm_nt(a, b):
    return lax.dot_general(a, b, NT, preferred_element_type=F32)


def turn(w):
    return w.astype(F32).T.astype(BF16)


def silu(v):
    u = 0.5 * v
    return (u + u * jnp.tanh(u)).astype(BF16)


def norm(y, axis):
    centre = y - jnp.mean(y, axis, keepdims=True)
    spread = jnp.mean(centre * centre, axis, keepdims=True)
    return centre * lax.rsqrt(spread + 1e-05)


def mlp_rows(first, w_second):
    return norm(mm(silu(first), w_second), 1)


def steps(rows):
    base = lax.broadcasted_iota(jnp.int32, (16, LANES), 0)
    return [(base + 16 * j).astype(F32).astype(BF16) for j in range(rows // 16)]


def hot(row, base, blocks):
    rows = 16 * len(blocks)
    n = row.shape[1]
    near = jnp.clip(jnp.broadcast_to(row, (16, n)) - base, -1, rows).astype(F32).astype(BF16)
    one = jnp.ones((16, n), BF16)
    zero = jnp.zeros((16, n), BF16)
    return jnp.concatenate(
        [jnp.where(jnp.concatenate([b] * (n // LANES), 1) == near, one, zero) for b in blocks], 0
    )


def ghosts_kernel(send, local, out, wide, picked):
    wide[...] = local[...].astype(F32)
    peers, slots = send.shape

    def one(p, _):
        for k in range(slots):
            picked[pl.ds(p * slots + k, 1), :] = wide[pl.ds(send[p, k], 1), :]
        return 0

    lax.fori_loop(0, peers, one, 0)
    out[...] = picked[...].astype(BF16)


def windows_after(step, base, high, rows):
    def run(k, _):
        step(base + rows * k)
        return 0

    lax.fori_loop(1, (high - base) // rows + 1, run, 0)


def chunk_list(rows):
    return [(c, min(CHUNK, rows - c)) for c in range(0, rows, CHUNK)]


def fine_first_kernel(
    count, bounds, edges, senders, receivers, local, w_edge, pre, agg, marks, rec, *, span
):
    nodes, width = local.shape
    tile = pre.shape[2]
    blocks = steps(CHUNK)
    small = steps(LANES)
    w = w_edge[0]
    w_send = turn(w[2 * width :])
    mine = local[...]
    rec[...] = mm(mine, w[width : 2 * width]).astype(BF16)
    tabs = [
        mm_nt(w_send, mine[c : c + CHUNK]).astype(BF16) for c in range(0, nodes, CHUNK)
    ]
    fixed = jnp.concatenate([turn(w[:width])] + tabs, 1)
    agg[...] = jnp.zeros_like(agg)
    live = count[0, 0]

    def one(t, _):
        later = []
        for p in range(0, tile, span):
            at = pl.multiple_of(t * tile + p, span)
            low = bounds[0, at]
            high = bounds[0, jnp.minimum(at + span, live) - 1]
            base = pl.multiple_of(jnp.minimum((low >> 4) << 4, nodes - LANES), 16)
            marks[0, t * (tile // span) + p // span] = base
            marks[1, t * (tile // span) + p // span] = high
            slots = at + lax.broadcasted_iota(jnp.int32, (1, span), 1)
            to = jnp.where(slots < live, receivers[:, pl.ds(at, span)], -1)
            left = jnp.concatenate([fixed, rec[pl.ds(base, LANES), :].T], 1)
            hots = []
            for n in range(0, span, SUB):
                row = senders[:, pl.ds(at + n, SUB)]
                hot_to = hot(to[:, n : n + SUB], base, small)
                right = [edges[pl.ds(at + n, SUB), :].T]
                right += [hot(row, c, blocks) for c in range(0, nodes, CHUNK)]
                full = mm(left, jnp.concatenate(right + [hot_to], 0))
                pre[t, :, p + n : p + n + SUB] = full.astype(BF16)
                hots.append(hot_to)
            agg[pl.ds(base, LANES), :] += mm(jnp.concatenate(hots, 1), edges[pl.ds(at, span), :])

            def more(start, at=at, to=to, p=p):
                begin = pl.multiple_of(jnp.minimum(start, nodes - LANES), 16)
                hot_far = hot(jnp.where(to >= start, to, -1), begin, small)
                extra = mm(rec[pl.ds(begin, LANES), :].T, hot_far)
                here = pre[t, :, p : p + span].astype(F32)
                pre[t, :, p : p + span] = (here + extra).astype(BF16)
                agg[pl.ds(begin, LANES), :] += mm(hot_far, edges[pl.ds(at, span), :])

            later.append((more, base, high, LANES))
        for item in later:
            windows_after(*item)
        return 0

    lax.fori_loop(0, (live + tile - 1) // tile, one, 0)


def fine_second_kernel(
    count, marks, pre, some, senders, receivers, local, ghosts, parents, w_edge, w_node, w_out,
    out, agg, *, span,
):
    tile = pre.shape[2]
    nodes, width = local.shape
    wide = 2 * span if tile % (2 * span) == 0 else span
    blocks = steps(CHUNK)
    pieces = chunk_list(ghosts.shape[0])
    w_send = turn(w_edge[0][2 * width :])
    tabs = [mm_nt(w_send, ghosts[pl.ds(c, n), :]).astype(BF16) for c, n in pieces]
    second = turn(w_out[0])
    agg[...] = some[...]
    live = count[0, 0]

    def one(t, _):
        later = []
        for p in range(0, tile, wide):
            at = pl.multiple_of(t * tile + p, wide)
            mark = t * (tile // span) + p // span
            base = pl.multiple_of(jnp.minimum(marks[0, mark], nodes - CHUNK), 16)
            high = marks[1, mark + wide // span - 1]
            slots = at + lax.broadcasted_iota(jnp.int32, (1, wide), 1)
            to = jnp.where(slots < live, receivers[:, pl.ds(at, wide)], -1)
            news = []
            for n in range(0, wide, SUB2):
                row = senders[:, pl.ds(at + n, SUB2)]
                first = pre[t, :, p + n : p + n + SUB2].astype(F32)
                for (c, k), tab in zip(pieces, tabs):
                    first += mm(tab, hot(row, nodes + c, blocks[: k // 16]))
                news.append(norm(mm(second, silu(first)), 0).astype(BF16))
            new = jnp.concatenate(news, 1)
            agg[pl.ds(base, CHUNK), :] += mm_nt(hot(to, base, blocks), new)

            def more(start, to=to, new=new):
                begin = pl.multiple_of(jnp.minimum(start, nodes - CHUNK), 16)
                far_to = jnp.where(to >= start, to, -1)
                agg[pl.ds(begin, CHUNK), :] += mm_nt(hot(far_to, begin, blocks), new)

            later.append((more, base, high, CHUNK))
        for item in later:
            windows_after(*item)
        return 0

    lax.fori_loop(0, (live + tile - 1) // tile, one, 0)
    mine = local[...]
    w = w_node[0]
    first = mm(mine, w[:width]) + mm(agg[...].astype(BF16), w[width:])
    out[pl.ds(0, nodes), :] = (mine.astype(F32) + mlp_rows(first, w_out[1])).astype(BF16)
    ids = parents[...]
    lines = nodes // LANES
    pads = out.shape[0] - nodes - 2 * lines
    parts = [ids[:, j * LANES : (j + 1) * LANES] for j in range(lines)]
    digits = [p >> 6 for p in parts] + [p & 63 for p in parts]
    digits = digits + [jnp.zeros((1, LANES), jnp.int32)] * pads
    out[pl.ds(nodes, 2 * lines + pads), :] = jnp.concatenate(digits, 0).astype(F32).astype(BF16)


def place(ids, owner_rows, piece, domains, group):
    owner = ids >> log2(owner_rows)
    within = ids & (owner_rows - 1)
    return (within >> log2(piece)) ^ group, owner * piece + (within & (piece - 1))


def pool_kernel(*refs, owner_rows, piece, domains, nodes):
    packs, out = refs[:-1], refs[-1]
    group = lax.axis_index("grp")
    lines = nodes // LANES
    blocks = steps(CHUNK)
    width = out.shape[1]
    chunk_rows = piece + 16
    spots = []
    fulls = []
    for pack in packs:
        tail = pack[pl.ds(nodes, pack.shape[0] - nodes), :].astype(F32).astype(jnp.int32)
        ids = jnp.concatenate(
            [(tail[j : j + 1] << 6) + tail[lines + j : lines + j + 1] for j in range(lines)], 1
        )
        side, spot = place(ids, owner_rows, piece, domains, group)
        spots.append(jnp.where(side == 0, spot, -1))
        fulls.append(
            jnp.concatenate([pack[pl.ds(0, nodes), :], jnp.ones((nodes, LANES), BF16)], 1)
        )
    eye = lax.broadcasted_iota(jnp.int32, (piece, LANES), 0) == lax.broadcasted_iota(
        jnp.int32, (piece, LANES), 1
    )
    lane_row = lax.broadcasted_iota(jnp.int32, (16, LANES), 0)
    for c in range(domains * piece // CHUNK):
        total = mm(hot(spots[0], c * CHUNK, blocks), fulls[0])
        for spot, full in zip(spots[1:], fulls[1:]):
            total += mm(hot(spot, c * CHUNK, blocks), full)
        for q in range(CHUNK // piece):
            base = (c * CHUNK // piece + q) * chunk_rows
            part = total[q * piece : (q + 1) * piece]
            out[pl.ds(base, piece), :] = part[:, :width].astype(BF16)
            many = jnp.sum(jnp.where(eye, part[:, width:], 0.0), 0, keepdims=True)
            high = jnp.floor(many * (1.0 / 256.0))
            low = many - 256.0 * high
            both = jnp.where(lane_row == 0, high, jnp.where(lane_row == 1, low, 0.0))
            out[pl.ds(base + piece, 16), :] = both.astype(BF16)


def coarse_mid_kernel(got, nodes, out, *, piece, domains):
    group = lax.axis_index("grp")
    chunk_rows = piece + 16
    parts = [got[pl.ds(s * chunk_rows, chunk_rows), :].astype(F32) for s in range(domains)]
    total = functools.reduce(jnp.add, parts)
    row = 256.0 * total[piece : piece + 1] + total[piece + 1 : piece + 2]
    eye = lax.broadcasted_iota(jnp.int32, (piece, LANES), 0) == lax.broadcasted_iota(
        jnp.int32, (piece, LANES), 1
    )
    many = jnp.sum(jnp.where(eye, jnp.broadcast_to(row, (piece, LANES)), 0.0), 1, keepdims=True)
    start = pl.multiple_of(group * piece, piece)
    mine = nodes[pl.ds(start, piece), :].astype(F32)
    mid = ((mine + total[:piece]) / (1.0 + many)).astype(BF16)
    for s in range(domains):
        out[pl.ds(s * piece, piece), :] = mid


def fill_table(parts, w, tab):
    per = parts[0].shape[0] // CHUNK
    for k, part in enumerate(parts):
        for c in range(per):
            tab[k * per + c] = mm_nt(w, part[pl.ds(c * CHUNK, CHUNK), :]).astype(BF16)


def look(tab, row, blocks, base):
    total = 0.0
    for c in range(0, tab.shape[0], 4):
        left = jnp.concatenate([tab[c + j] for j in range(4)], 1)
        right = [hot(row, base + (c + j) * CHUNK, blocks) for j in range(4)]
        total += mm(left, jnp.concatenate(right, 0))
    return total


def edge_range(receivers, low, piece):
    every = receivers[...]
    start = jnp.sum((every < low).astype(jnp.int32))
    end = jnp.sum((every < low + piece).astype(jnp.int32))
    return (start >> log2(LANES)) << log2(LANES), end


def edge_tile(t, begin, tile, senders, receivers, low, owner_rows, piece, domains, group):
    wanted = begin + t * tile
    at = pl.multiple_of(jnp.minimum(wanted, senders.shape[1] - tile), LANES)
    here = pl.ds(at, tile)
    side, spot = place(senders[:, here], owner_rows, piece, domains, group)
    slots = at + lax.broadcasted_iota(jnp.int32, (1, tile), 1)
    to = jnp.where(slots >= wanted, receivers[:, here] - low, -1)
    return at, side * (domains * piece) + spot, to


def coarse_first_kernel(*refs, near_parts, owner_rows, piece, domains):
    parts = refs[:near_parts]
    edges, senders, receivers, w_edge = refs[near_parts : near_parts + 4]
    pre, agg, tab = refs[near_parts + 4 :]
    group = lax.axis_index("grp")
    domain = lax.axis_index("dom")
    width = edges.shape[1]
    tile = pre.shape[2]
    blocks = steps(CHUNK)
    small = steps(piece)
    w = w_edge[1]
    fill_table(parts, turn(w[2 * width :]), tab)
    mine = parts[0][pl.ds(pl.multiple_of(domain * piece, piece), piece), :]
    rec = mm_nt(turn(w[width : 2 * width]), mine).astype(BF16)
    mix = jnp.concatenate([turn(w[:width]), rec], 1)
    agg[...] = jnp.zeros_like(agg)
    low = group * piece
    begin, end = edge_range(receivers, low, piece)

    def one(t, _):
        at, row, to = edge_tile(
            t, begin, tile, senders, receivers, low, owner_rows, piece, domains, group
        )
        hots = []
        for n in range(0, tile, SUB):
            hot_to = hot(to[:, n : n + SUB], 0, small)
            flat = edges[pl.ds(at + n, SUB), :].T
            first = mm(mix, jnp.concatenate([flat, hot_to], 0))
            first += look(tab, row[:, n : n + SUB], blocks, 0)
            pre[t, :, n : n + SUB] = first.astype(BF16)
            hots.append(hot_to)
        agg[...] += mm(jnp.concatenate(hots, 1), edges[pl.ds(at, tile), :])
        return 0

    lax.fori_loop(0, (end - begin + tile - 1) // tile, one, 0)


def coarse_second_kernel(*refs, far_parts, owner_rows, piece, domains):
    own, *parts = refs[: far_parts + 1]
    pre, some, senders, receivers, w_edge, w_node, w_out = refs[far_parts + 1 : far_parts + 8]
    out, tab, agg = refs[far_parts + 8 :]
    group = lax.axis_index("grp")
    domain = lax.axis_index("dom")
    width = own.shape[1]
    tile = pre.shape[2]
    blocks = steps(CHUNK)
    small = steps(piece)
    fill_table(parts, turn(w_edge[1][2 * width :]), tab)
    mine = own[pl.ds(pl.multiple_of(domain * piece, piece), piece), :]
    second = turn(w_out[2])
    agg[...] = some[...]
    low = group * piece
    begin, end = edge_range(receivers, low, piece)
    base = far_parts * domains * piece

    def one(t, _):
        _, row, to = edge_tile(
            t, begin, tile, senders, receivers, low, owner_rows, piece, domains, group
        )
        news = []
        for n in range(0, tile, SUB):
            first = pre[t, :, n : n + SUB].astype(F32)
            first += look(tab, row[:, n : n + SUB], blocks, base)
            news.append(norm(mm(second, silu(first)), 0).astype(BF16))
        agg[...] += mm_nt(hot(to, 0, small), jnp.concatenate(news, 1))
        return 0

    lax.fori_loop(0, (end - begin + tile - 1) // tile, one, 0)
    wn = w_node[1]
    first = mm(mine, wn[:width]) + mm(agg[...].astype(BF16), wn[width:])
    new = (mine.astype(F32) + mlp_rows(first, w_out[3])).astype(BF16)
    for s in range(domains):
        out[pl.ds(s * piece, piece), :] = new


def return_first_kernel(*refs, near_parts, owner_rows, piece, domains, nodes):
    parts = refs[:near_parts]
    packed, parents, w_node = refs[near_parts : near_parts + 3]
    pre, tab = refs[near_parts + 3 :]
    width = packed.shape[1]
    w = w_node[2]
    fill_table(parts, turn(w[width:]), tab)
    side, spot = place(parents[...], owner_rows, piece, domains, lax.axis_index("grp"))
    row = side * (domains * piece) + spot
    first = mm_nt(turn(w[:width]), packed[pl.ds(0, nodes), :])
    blocks = steps(CHUNK)
    for c in range(tab.shape[0]):
        first += mm(tab[c], hot(row, c * CHUNK, blocks))
    pre[...] = first


def return_second_kernel(*refs, groups, owner_rows, piece, domains, nodes):
    parts = refs[:groups]
    pre, packed, parents, w_node, w_out = refs[groups : groups + 5]
    out, coarse, tab = refs[groups + 5 :]
    group = lax.axis_index("grp")
    domain = lax.axis_index("dom")
    width = out.shape[1]
    blocks = steps(CHUNK)
    start = pl.multiple_of(domain * piece, piece)
    for side in range(groups):
        to = pl.multiple_of((group ^ side) * piece, piece)
        coarse[pl.ds(to, piece), :] = parts[side][pl.ds(start, piece), :]
    fill_table(parts[groups // 2 :], turn(w_node[2][width:]), tab)
    side, spot = place(parents[...], owner_rows, piece, domains, group)
    row = side * (domains * piece) + spot
    first = pre[...]
    for c in range(tab.shape[0]):
        first += mm(tab[c], hot(row, (c + tab.shape[0]) * CHUNK, blocks))
    y = norm(mm(turn(w_out[4]), silu(first)), 0)
    out[...] = (packed[pl.ds(0, nodes), :].astype(F32) + y.T).astype(BF16)


def spread(x, groups, bit):
    held = {0: x}
    while bit:
        for k in sorted(held):
            held[k | bit] = lax.ppermute(
                held[k], "grp", [(i, i ^ bit) for i in range(groups)]
            )
        bit >>= 1
    return [near(held[k]) for k in sorted(held)]


def spread_over(x, groups, work):
    bit = groups >> 1
    other = lax.ppermute(x, "grp", [(i, i ^ bit) for i in range(groups)])
    parts = spread(x, groups, bit >> 1)
    done = work(parts)
    other, done = lax.optimization_barrier((other, done))
    return parts, spread(other, groups, bit >> 1), done


def near(x):
    return pltpu.with_memory_space_constraint(x, pltpu.VMEM)


def far(x):
    return pltpu.with_memory_space_constraint(x, pltpu.HBM)


def swap(x):
    return lax.all_to_all(x, "dom", split_axis=0, concat_axis=0, tiled=True)


def per_device(
    fine_nodes,
    fine_edges,
    fine_senders,
    fine_receivers,
    edge_count,
    ghost_send,
    fine_parent,
    coarse_nodes,
    coarse_edges,
    coarse_senders,
    coarse_receivers,
    edge_in,
    node_in,
    mlp_out,
):
    domains = lax.axis_size("dom")
    groups = lax.axis_size("grp")
    local = fine_nodes[0]
    edges = fine_edges[0]
    nodes, width = local.shape
    slots = edges.shape[0]
    owner_rows = coarse_nodes.shape[0]
    coarse_slots = coarse_edges.shape[0]
    piece = owner_rows // groups
    ghosts = ghost_send.shape[1] * ghost_send.shape[2]
    sizes = dict(owner_rows=owner_rows, piece=piece, domains=domains)
    assert nodes % CHUNK == 0 and CHUNK % piece == 0 and piece <= LANES
    assert owner_rows * domains <= 1 << 14
    span = max(t for t in (256, 512, 768) if slots % t == 0)
    tile = max(span * k for k in (1, 2, 4) if slots % (span * k) == 0)
    ctile = max(t for t in (256, 512, 1280) if coarse_slots >= t)
    assert coarse_slots % LANES == 0 and groups % 2 == 0

    params = pltpu.CompilerParams(vmem_limit_bytes=24 << 20)
    w_edge = near(edge_in)
    w_node = near(node_in)
    w_out = near(mlp_out)
    parents = near(fine_parent)

    outgoing = pl.pallas_call(
        ghosts_kernel,
        out_shape=pltpu.VMEM((ghosts, width), BF16),
        in_specs=[SMEM, VMEM],
        out_specs=VMEM,
        scratch_shapes=[pltpu.VMEM((nodes, width), F32), pltpu.VMEM((ghosts, width), F32)],
        compiler_params=params,
        name="ghosts",
    )(far(ghost_send[0]), far(local))
    incoming = near(swap(outgoing))

    tiles = slots // tile
    pre, some, marks = pl.pallas_call(
        functools.partial(fine_first_kernel, span=span),
        out_shape=(
            pltpu.VMEM((tiles, width, tile), BF16),
            pltpu.VMEM((nodes, width), F32),
            pltpu.HBM((2, slots // span), jnp.int32),
        ),
        in_specs=[SMEM, SMEM] + [VMEM] * 5,
        out_specs=(VMEM, VMEM, SMEM),
        scratch_shapes=[pltpu.VMEM((nodes, width), BF16)],
        compiler_params=params,
        cost_estimate=pl.CostEstimate(
            flops=2 * slots * width * (nodes + 2 * width), transcendentals=0, bytes_accessed=0
        ),
        name="fine_first",
    )(
        edge_count, far(fine_receivers), far(edges), far(fine_senders), far(fine_receivers),
        far(local), far(edge_in),
    )

    pack_rows = nodes + -(-2 * (nodes // LANES) // 16) * 16
    packed = pl.pallas_call(
        functools.partial(fine_second_kernel, span=span),
        out_shape=pltpu.VMEM((pack_rows, width), BF16),
        in_specs=[SMEM, SMEM] + [VMEM] * 10,
        out_specs=VMEM,
        scratch_shapes=[pltpu.VMEM((nodes, width), F32)],
        compiler_params=params,
        name="fine_second",
    )(
        edge_count, far(marks), near(pre), near(some), far(fine_senders), far(fine_receivers),
        near(local), incoming, far(fine_parent), w_edge, w_node, w_out,
    )
    packed = near(packed)

    packs = spread(packed, groups, groups >> 1)
    pooled = pl.pallas_call(
        functools.partial(pool_kernel, nodes=nodes, **sizes),
        out_shape=pltpu.VMEM((domains * (piece + 16), width), BF16),
        in_specs=[VMEM] * groups,
        out_specs=VMEM,
        compiler_params=params,
        name="pool",
    )(*packs)
    got = near(swap(pooled))
    copies = pltpu.VMEM((domains * piece, width), BF16)
    mid = pl.pallas_call(
        functools.partial(coarse_mid_kernel, piece=piece, domains=domains),
        out_shape=copies,
        in_specs=[VMEM] * 2,
        out_specs=VMEM,
        compiler_params=params,
        name="coarse_mid",
    )(got, near(coarse_nodes))
    half = groups // 2
    table = pltpu.VMEM((owner_rows * domains // CHUNK // 2, width, CHUNK), BF16)
    ctiles = -(-(coarse_slots + LANES) // ctile)
    csenders = near(coarse_senders[None])
    creceivers = near(coarse_receivers[None])
    cost = pl.CostEstimate(flops=1 << 31, transcendentals=0, bytes_accessed=0)

    def coarse_first(parts):
        return pl.pallas_call(
            functools.partial(coarse_first_kernel, near_parts=half, **sizes),
            out_shape=(pltpu.VMEM((ctiles, width, ctile), BF16), pltpu.VMEM((piece, width), F32)),
            in_specs=[VMEM] * (half + 4),
            out_specs=(VMEM, VMEM),
            scratch_shapes=[table],
            compiler_params=params,
            cost_estimate=cost,
            name="coarse_first",
        )(*parts, far(coarse_edges), csenders, creceivers, w_edge)

    closer, others, (cpre, csome) = spread_over(swap(mid), groups, coarse_first)
    coarse = pl.pallas_call(
        functools.partial(coarse_second_kernel, far_parts=half, **sizes),
        out_shape=copies,
        in_specs=[VMEM] * (half + 8),
        out_specs=VMEM,
        scratch_shapes=[table, pltpu.VMEM((piece, width), F32)],
        compiler_params=params,
        name="coarse_second",
    )(
        closer[0], *others, near(cpre), near(csome), csenders, creceivers, w_edge, w_node, w_out,
    )

    def return_first(parts):
        return pl.pallas_call(
            functools.partial(return_first_kernel, near_parts=half, nodes=nodes, **sizes),
            out_shape=pltpu.VMEM((width, nodes), F32),
            in_specs=[VMEM] * (half + 3),
            out_specs=VMEM,
            scratch_shapes=[table],
            compiler_params=params,
            cost_estimate=cost,
            name="back_first",
        )(*parts, packed, parents, w_node)

    closer, others, pre_out = spread_over(swap(coarse), groups, return_first)
    fine_out, coarse_out = pl.pallas_call(
        functools.partial(return_second_kernel, groups=groups, nodes=nodes, **sizes),
        out_shape=(
            jax.ShapeDtypeStruct((nodes, width), BF16),
            jax.ShapeDtypeStruct((owner_rows, width), BF16),
        ),
        in_specs=[VMEM] * (groups + 5),
        out_specs=(VMEM, VMEM),
        scratch_shapes=[table],
        compiler_params=params,
        name="back_second",
    )(*closer, *others, near(pre_out), packed, parents, w_node, w_out)
    return (fine_out[None], coarse_out)


def solution(mesh):
    placed = (
        P("grp", "dom", None),
        P("grp", "dom", None),
        P("grp", "dom"),
        P("grp", "dom"),
        P("grp", "dom"),
        P("grp", "dom", None),
        P("grp", "dom"),
        P("dom", None),
        P("dom", None),
        P("dom"),
        P("dom"),
        P(),
        P(),
        P(),
    )
    return jax.shard_map(
        per_device,
        mesh=mesh,
        in_specs=placed,
        out_specs=(P("grp", "dom", None), P("dom", None)),
        check_vma=False,
    )
```

```python
import functools

import jax
import jax.numpy as jnp
from jax import lax
from jax.experimental import pallas as pl
from jax.experimental.pallas import tpu as pltpu
from jax.sharding import PartitionSpec as P


F32 = jnp.float32
BF16 = jnp.bfloat16
NT = (((1,), (1,)), ((), ()))
CHUNK = 256
SUB = 256
SUB2 = 256
LANES = 128
VMEM = pl.BlockSpec(memory_space=pltpu.VMEM)
SMEM = pl.BlockSpec(memory_space=pltpu.SMEM)


def log2(n):
    bits = n.bit_length() - 1
    assert 1 << bits == n
    return bits


def mm(a, b):
    return jnp.dot(a, b, preferred_element_type=F32)


def mm_nt(a, b):
    return lax.dot_general(a, b, NT, preferred_element_type=F32)


def turn(w):
    return w.astype(F32).T.astype(BF16)


def silu(v):
    u = 0.5 * v
    return (u + u * jnp.tanh(u)).astype(BF16)


def norm(y, axis):
    centre = y - jnp.mean(y, axis, keepdims=True)
    spread = jnp.mean(centre * centre, axis, keepdims=True)
    return centre * lax.rsqrt(spread + 1e-05)


def mlp_rows(first, w_second):
    return norm(mm(silu(first), w_second), 1)


def steps(rows):
    base = lax.broadcasted_iota(jnp.int32, (16, LANES), 0)
    return [(base + 16 * j).astype(F32).astype(BF16) for j in range(rows // 16)]


def hot(row, base, blocks):
    rows = 16 * len(blocks)
    n = row.shape[1]
    near = jnp.clip(jnp.broadcast_to(row, (16, n)) - base, -1, rows).astype(F32).astype(BF16)
    one = jnp.ones((16, n), BF16)
    zero = jnp.zeros((16, n), BF16)
    return jnp.concatenate(
        [jnp.where(jnp.concatenate([b] * (n // LANES), 1) == near, one, zero) for b in blocks], 0
    )


def ghosts_kernel(send, local, out, wide, picked):
    wide[...] = local[...].astype(F32)
    peers, slots = send.shape

    def one(p, _):
        for k in range(slots):
            picked[pl.ds(p * slots + k, 1), :] = wide[pl.ds(send[p, k], 1), :]
        return 0

    lax.fori_loop(0, peers, one, 0)
    out[...] = picked[...].astype(BF16)


def windows_after(step, base, high, rows):
    def run(k, _):
        step(base + rows * k)
        return 0

    lax.fori_loop(1, (high - base) // rows + 1, run, 0)


def chunk_list(rows):
    return [(c, min(CHUNK, rows - c)) for c in range(0, rows, CHUNK)]


def fine_first_kernel(
    count, bounds, edges, senders, receivers, local, w_edge, pre, agg, marks, rec, *, span
):
    nodes, width = local.shape
    tile = pre.shape[2]
    blocks = steps(CHUNK)
    small = steps(LANES)
    w = w_edge[0]
    w_send = turn(w[2 * width :])
    mine = local[...]
    rec[...] = mm(mine, w[width : 2 * width]).astype(BF16)
    tabs = [
        mm_nt(w_send, mine[c : c + CHUNK]).astype(BF16) for c in range(0, nodes, CHUNK)
    ]
    fixed = jnp.concatenate([turn(w[:width])] + tabs, 1)
    agg[...] = jnp.zeros_like(agg)
    live = count[0, 0]

    def one(t, _):
        later = []
        for p in range(0, tile, span):
            at = pl.multiple_of(t * tile + p, span)
            low = bounds[0, at]
            high = bounds[0, jnp.minimum(at + span, live) - 1]
            base = pl.multiple_of(jnp.minimum((low >> 4) << 4, nodes - LANES), 16)
            marks[0, t * (tile // span) + p // span] = base
            marks[1, t * (tile // span) + p // span] = high
            slots = at + lax.broadcasted_iota(jnp.int32, (1, span), 1)
            to = jnp.where(slots < live, receivers[:, pl.ds(at, span)], -1)
            left = jnp.concatenate([fixed, rec[pl.ds(base, LANES), :].T], 1)
            hots = []
            for n in range(0, span, SUB):
                row = senders[:, pl.ds(at + n, SUB)]
                hot_to = hot(to[:, n : n + SUB], base, small)
                right = [edges[pl.ds(at + n, SUB), :].T]
                right += [hot(row, c, blocks) for c in range(0, nodes, CHUNK)]
                full = mm(left, jnp.concatenate(right + [hot_to], 0))
                pre[t, :, p + n : p + n + SUB] = full.astype(BF16)
                hots.append(hot_to)
            agg[pl.ds(base, LANES), :] += mm(jnp.concatenate(hots, 1), edges[pl.ds(at, span), :])

            def more(start, at=at, to=to, p=p):
                begin = pl.multiple_of(jnp.minimum(start, nodes - LANES), 16)
                hot_far = hot(jnp.where(to >= start, to, -1), begin, small)
                extra = mm(rec[pl.ds(begin, LANES), :].T, hot_far)
                here = pre[t, :, p : p + span].astype(F32)
                pre[t, :, p : p + span] = (here + extra).astype(BF16)
                agg[pl.ds(begin, LANES), :] += mm(hot_far, edges[pl.ds(at, span), :])

            later.append((more, base, high, LANES))
        for item in later:
            windows_after(*item)
        return 0

    lax.fori_loop(0, (live + tile - 1) // tile, one, 0)


def fine_second_kernel(
    count, marks, pre, some, senders, receivers, local, ghosts, parents, w_edge, w_node, w_out,
    out, agg, *, span,
):
    tile = pre.shape[2]
    nodes, width = local.shape
    wide = 2 * span if tile % (2 * span) == 0 else span
    blocks = steps(CHUNK)
    pieces = chunk_list(ghosts.shape[0])
    w_send = turn(w_edge[0][2 * width :])
    tabs = [mm_nt(w_send, ghosts[pl.ds(c, n), :]).astype(BF16) for c, n in pieces]
    second = turn(w_out[0])
    agg[...] = some[...]
    live = count[0, 0]

    def one(t, _):
        later = []
        for p in range(0, tile, wide):
            at = pl.multiple_of(t * tile + p, wide)
            mark = t * (tile // span) + p // span
            base = pl.multiple_of(jnp.minimum(marks[0, mark], nodes - CHUNK), 16)
            high = marks[1, mark + wide // span - 1]
            slots = at + lax.broadcasted_iota(jnp.int32, (1, wide), 1)
            to = jnp.where(slots < live, receivers[:, pl.ds(at, wide)], -1)
            news = []
            for n in range(0, wide, SUB2):
                row = senders[:, pl.ds(at + n, SUB2)]
                first = pre[t, :, p + n : p + n + SUB2].astype(F32)
                for (c, k), tab in zip(pieces, tabs):
                    first += mm(tab, hot(row, nodes + c, blocks[: k // 16]))
                news.append(norm(mm(second, silu(first)), 0).astype(BF16))
            new = jnp.concatenate(news, 1)
            agg[pl.ds(base, CHUNK), :] += mm_nt(hot(to, base, blocks), new)

            def more(start, to=to, new=new):
                begin = pl.multiple_of(jnp.minimum(start, nodes - CHUNK), 16)
                far_to = jnp.where(to >= start, to, -1)
                agg[pl.ds(begin, CHUNK), :] += mm_nt(hot(far_to, begin, blocks), new)

            later.append((more, base, high, CHUNK))
        for item in later:
            windows_after(*item)
        return 0

    lax.fori_loop(0, (live + tile - 1) // tile, one, 0)
    mine = local[...]
    w = w_node[0]
    first = mm(mine, w[:width]) + mm(agg[...].astype(BF16), w[width:])
    out[pl.ds(0, nodes), :] = (mine.astype(F32) + mlp_rows(first, w_out[1])).astype(BF16)
    ids = parents[...]
    lines = nodes // LANES
    pads = out.shape[0] - nodes - 2 * lines
    parts = [ids[:, j * LANES : (j + 1) * LANES] for j in range(lines)]
    digits = [p >> 6 for p in parts] + [p & 63 for p in parts]
    digits = digits + [jnp.zeros((1, LANES), jnp.int32)] * pads
    out[pl.ds(nodes, 2 * lines + pads), :] = jnp.concatenate(digits, 0).astype(F32).astype(BF16)


def place(ids, owner_rows, piece, group):
    owner = ids >> log2(owner_rows)
    within = ids & (owner_rows - 1)
    return (within >> log2(piece)) ^ group, owner * piece + (within & (piece - 1))


def pool_kernel(*refs, owner_rows, piece, domains, nodes):
    packs, out = refs[:-1], refs[-1]
    group = lax.axis_index("grp")
    lines = nodes // LANES
    blocks = steps(CHUNK)
    width = out.shape[1]
    chunk_rows = piece + 16
    spots = []
    fulls = []
    for pack in packs:
        tail = pack[pl.ds(nodes, pack.shape[0] - nodes), :].astype(F32).astype(jnp.int32)
        ids = jnp.concatenate(
            [(tail[j : j + 1] << 6) + tail[lines + j : lines + j + 1] for j in range(lines)], 1
        )
        side, spot = place(ids, owner_rows, piece, group)
        spots.append(jnp.where(side == 0, spot, -1))
        fulls.append(
            jnp.concatenate([pack[pl.ds(0, nodes), :], jnp.ones((nodes, LANES), BF16)], 1)
        )
    eye = lax.broadcasted_iota(jnp.int32, (piece, LANES), 0) == lax.broadcasted_iota(
        jnp.int32, (piece, LANES), 1
    )
    lane_row = lax.broadcasted_iota(jnp.int32, (16, LANES), 0)
    for c in range(domains * piece // CHUNK):
        total = mm(hot(spots[0], c * CHUNK, blocks), fulls[0])
        for spot, full in zip(spots[1:], fulls[1:]):
            total += mm(hot(spot, c * CHUNK, blocks), full)
        for q in range(CHUNK // piece):
            base = (c * CHUNK // piece + q) * chunk_rows
            part = total[q * piece : (q + 1) * piece]
            out[pl.ds(base, piece), :] = part[:, :width].astype(BF16)
            many = jnp.sum(jnp.where(eye, part[:, width:], 0.0), 0, keepdims=True)
            high = jnp.floor(many * (1.0 / 256.0))
            low = many - 256.0 * high
            both = jnp.where(lane_row == 0, high, jnp.where(lane_row == 1, low, 0.0))
            out[pl.ds(base + piece, 16), :] = both.astype(BF16)


def coarse_mid_kernel(got, nodes, out, *, piece, domains):
    group = lax.axis_index("grp")
    chunk_rows = piece + 16
    parts = [got[pl.ds(s * chunk_rows, chunk_rows), :].astype(F32) for s in range(domains)]
    total = functools.reduce(jnp.add, parts)
    row = 256.0 * total[piece : piece + 1] + total[piece + 1 : piece + 2]
    eye = lax.broadcasted_iota(jnp.int32, (piece, LANES), 0) == lax.broadcasted_iota(
        jnp.int32, (piece, LANES), 1
    )
    many = jnp.sum(jnp.where(eye, jnp.broadcast_to(row, (piece, LANES)), 0.0), 1, keepdims=True)
    start = pl.multiple_of(group * piece, piece)
    mine = nodes[pl.ds(start, piece), :].astype(F32)
    mid = ((mine + total[:piece]) / (1.0 + many)).astype(BF16)
    for s in range(domains):
        out[pl.ds(s * piece, piece), :] = mid


def fill_table(parts, w, tab):
    per = parts[0].shape[0] // CHUNK
    for k, part in enumerate(parts):
        for c in range(per):
            tab[k * per + c] = mm_nt(w, part[pl.ds(c * CHUNK, CHUNK), :]).astype(BF16)


def look(tab, row, blocks, base):
    total = 0.0
    for c in range(0, tab.shape[0], 4):
        left = jnp.concatenate([tab[c + j] for j in range(4)], 1)
        right = [hot(row, base + (c + j) * CHUNK, blocks) for j in range(4)]
        total += mm(left, jnp.concatenate(right, 0))
    return total


def edge_range(receivers, low, piece):
    every = receivers[...]
    start = jnp.sum((every < low).astype(jnp.int32))
    end = jnp.sum((every < low + piece).astype(jnp.int32))
    return (start >> log2(LANES)) << log2(LANES), end


def edge_tile(t, begin, tile, senders, receivers, low, owner_rows, piece, domains, group):
    wanted = begin + t * tile
    at = pl.multiple_of(jnp.minimum(wanted, senders.shape[1] - tile), LANES)
    here = pl.ds(at, tile)
    side, spot = place(senders[:, here], owner_rows, piece, group)
    slots = at + lax.broadcasted_iota(jnp.int32, (1, tile), 1)
    to = jnp.where(slots >= wanted, receivers[:, here] - low, -1)
    return at, side * (domains * piece) + spot, to


def coarse_first_kernel(*refs, near_parts, owner_rows, piece, domains):
    parts = refs[:near_parts]
    edges, senders, receivers, w_edge = refs[near_parts : near_parts + 4]
    pre, agg, tab = refs[near_parts + 4 :]
    group = lax.axis_index("grp")
    domain = lax.axis_index("dom")
    width = edges.shape[1]
    tile = pre.shape[2]
    blocks = steps(CHUNK)
    small = steps(piece)
    w = w_edge[1]
    fill_table(parts, turn(w[2 * width :]), tab)
    mine = parts[0][pl.ds(pl.multiple_of(domain * piece, piece), piece), :]
    rec = mm_nt(turn(w[width : 2 * width]), mine).astype(BF16)
    mix = jnp.concatenate([turn(w[:width]), rec], 1)
    agg[...] = jnp.zeros_like(agg)
    low = group * piece
    begin, end = edge_range(receivers, low, piece)

    def one(t, _):
        at, row, to = edge_tile(
            t, begin, tile, senders, receivers, low, owner_rows, piece, domains, group
        )
        hots = []
        for n in range(0, tile, SUB):
            hot_to = hot(to[:, n : n + SUB], 0, small)
            flat = edges[pl.ds(at + n, SUB), :].T
            first = mm(mix, jnp.concatenate([flat, hot_to], 0))
            first += look(tab, row[:, n : n + SUB], blocks, 0)
            pre[t, :, n : n + SUB] = first.astype(BF16)
            hots.append(hot_to)
        agg[...] += mm(jnp.concatenate(hots, 1), edges[pl.ds(at, tile), :])
        return 0

    lax.fori_loop(0, (end - begin + tile - 1) // tile, one, 0)


def coarse_second_kernel(*refs, far_parts, owner_rows, piece, domains):
    own, *parts = refs[: far_parts + 1]
    pre, some, senders, receivers, w_edge, w_node, w_out = refs[far_parts + 1 : far_parts + 8]
    out, tab, agg = refs[far_parts + 8 :]
    group = lax.axis_index("grp")
    domain = lax.axis_index("dom")
    width = own.shape[1]
    tile = pre.shape[2]
    blocks = steps(CHUNK)
    small = steps(piece)
    fill_table(parts, turn(w_edge[1][2 * width :]), tab)
    mine = own[pl.ds(pl.multiple_of(domain * piece, piece), piece), :]
    second = turn(w_out[2])
    agg[...] = some[...]
    low = group * piece
    begin, end = edge_range(receivers, low, piece)
    base = far_parts * domains * piece

    def one(t, _):
        _, row, to = edge_tile(
            t, begin, tile, senders, receivers, low, owner_rows, piece, domains, group
        )
        news = []
        for n in range(0, tile, SUB):
            first = pre[t, :, n : n + SUB].astype(F32)
            first += look(tab, row[:, n : n + SUB], blocks, base)
            news.append(norm(mm(second, silu(first)), 0).astype(BF16))
        agg[...] += mm_nt(hot(to, 0, small), jnp.concatenate(news, 1))
        return 0

    lax.fori_loop(0, (end - begin + tile - 1) // tile, one, 0)
    wn = w_node[1]
    first = mm(mine, wn[:width]) + mm(agg[...].astype(BF16), wn[width:])
    new = (mine.astype(F32) + mlp_rows(first, w_out[3])).astype(BF16)
    for s in range(domains):
        out[pl.ds(s * piece, piece), :] = new


def return_first_kernel(*refs, near_parts, owner_rows, piece, domains, nodes):
    parts = refs[:near_parts]
    packed, parents, w_node = refs[near_parts : near_parts + 3]
    pre, tab = refs[near_parts + 3 :]
    width = packed.shape[1]
    w = w_node[2]
    fill_table(parts, turn(w[width:]), tab)
    side, spot = place(parents[...], owner_rows, piece, lax.axis_index("grp"))
    row = side * (domains * piece) + spot
    first = mm_nt(turn(w[:width]), packed[pl.ds(0, nodes), :])
    blocks = steps(CHUNK)
    for c in range(tab.shape[0]):
        first += mm(tab[c], hot(row, c * CHUNK, blocks))
    pre[...] = first


def return_second_kernel(*refs, groups, owner_rows, piece, domains, nodes):
    parts = refs[:groups]
    pre, packed, parents, w_node, w_out = refs[groups : groups + 5]
    out, coarse, tab = refs[groups + 5 :]
    group = lax.axis_index("grp")
    domain = lax.axis_index("dom")
    width = out.shape[1]
    blocks = steps(CHUNK)
    start = pl.multiple_of(domain * piece, piece)
    for side in range(groups):
        to = pl.multiple_of((group ^ side) * piece, piece)
        coarse[pl.ds(to, piece), :] = parts[side][pl.ds(start, piece), :]
    fill_table(parts[groups // 2 :], turn(w_node[2][width:]), tab)
    side, spot = place(parents[...], owner_rows, piece, group)
    row = side * (domains * piece) + spot
    first = pre[...]
    for c in range(tab.shape[0]):
        first += mm(tab[c], hot(row, (c + tab.shape[0]) * CHUNK, blocks))
    y = norm(mm(turn(w_out[4]), silu(first)), 0)
    out[...] = (packed[pl.ds(0, nodes), :].astype(F32) + y.T).astype(BF16)


def spread(x, groups, bit):
    held = {0: x}
    while bit:
        for k in sorted(held):
            held[k | bit] = lax.ppermute(
                held[k], "grp", [(i, i ^ bit) for i in range(groups)]
            )
        bit >>= 1
    return [near(held[k]) for k in sorted(held)]


def spread_over(x, groups, work):
    bit = groups >> 1
    other = lax.ppermute(x, "grp", [(i, i ^ bit) for i in range(groups)])
    parts = spread(x, groups, bit >> 1)
    done = work(parts)
    other, done = lax.optimization_barrier((other, done))
    return parts, spread(other, groups, bit >> 1), done


def near(x):
    return pltpu.with_memory_space_constraint(x, pltpu.VMEM)


def far(x):
    return pltpu.with_memory_space_constraint(x, pltpu.HBM)


def swap(x):
    return lax.all_to_all(x, "dom", split_axis=0, concat_axis=0, tiled=True)


def per_device(
    fine_nodes,
    fine_edges,
    fine_senders,
    fine_receivers,
    edge_count,
    ghost_send,
    fine_parent,
    coarse_nodes,
    coarse_edges,
    coarse_senders,
    coarse_receivers,
    edge_in,
    node_in,
    mlp_out,
):
    domains = lax.axis_size("dom")
    groups = lax.axis_size("grp")
    local = fine_nodes[0]
    edges = fine_edges[0]
    nodes, width = local.shape
    slots = edges.shape[0]
    owner_rows = coarse_nodes.shape[0]
    coarse_slots = coarse_edges.shape[0]
    piece = owner_rows // groups
    ghosts = ghost_send.shape[1] * ghost_send.shape[2]
    sizes = dict(owner_rows=owner_rows, piece=piece, domains=domains)
    assert nodes % CHUNK == 0 and CHUNK % piece == 0 and piece <= LANES
    assert owner_rows * domains <= 1 << 14
    span = max(t for t in (256, 512, 768) if slots % t == 0)
    tile = max(span * k for k in (1, 2, 4) if slots % (span * k) == 0)
    ctile = max(t for t in (256, 512, 1280) if coarse_slots >= t)
    assert coarse_slots % LANES == 0 and groups % 2 == 0

    params = pltpu.CompilerParams(vmem_limit_bytes=24 << 20)
    w_edge = near(edge_in)
    w_node = near(node_in)
    w_out = near(mlp_out)
    parents = near(fine_parent)

    outgoing = pl.pallas_call(
        ghosts_kernel,
        out_shape=pltpu.VMEM((ghosts, width), BF16),
        in_specs=[SMEM, VMEM],
        out_specs=VMEM,
        scratch_shapes=[pltpu.VMEM((nodes, width), F32), pltpu.VMEM((ghosts, width), F32)],
        compiler_params=params,
        name="ghosts",
    )(far(ghost_send[0]), far(local))
    incoming = near(swap(outgoing))

    tiles = slots // tile
    pre, some, marks = pl.pallas_call(
        functools.partial(fine_first_kernel, span=span),
        out_shape=(
            pltpu.VMEM((tiles, width, tile), BF16),
            pltpu.VMEM((nodes, width), F32),
            pltpu.HBM((2, slots // span), jnp.int32),
        ),
        in_specs=[SMEM, SMEM] + [VMEM] * 5,
        out_specs=(VMEM, VMEM, SMEM),
        scratch_shapes=[pltpu.VMEM((nodes, width), BF16)],
        compiler_params=params,
        cost_estimate=pl.CostEstimate(
            flops=2 * slots * width * (nodes + 2 * width), transcendentals=0, bytes_accessed=0
        ),
        name="fine_first",
    )(
        edge_count, far(fine_receivers), far(edges), far(fine_senders), far(fine_receivers),
        far(local), far(edge_in),
    )

    pack_rows = nodes + -(-2 * (nodes // LANES) // 16) * 16
    packed = pl.pallas_call(
        functools.partial(fine_second_kernel, span=span),
        out_shape=pltpu.VMEM((pack_rows, width), BF16),
        in_specs=[SMEM, SMEM] + [VMEM] * 10,
        out_specs=VMEM,
        scratch_shapes=[pltpu.VMEM((nodes, width), F32)],
        compiler_params=params,
        name="fine_second",
    )(
        edge_count, far(marks), near(pre), near(some), far(fine_senders), far(fine_receivers),
        near(local), incoming, far(fine_parent), w_edge, w_node, w_out,
    )
    packed = near(packed)

    packs = spread(packed, groups, groups >> 1)
    pooled = pl.pallas_call(
        functools.partial(pool_kernel, nodes=nodes, **sizes),
        out_shape=pltpu.VMEM((domains * (piece + 16), width), BF16),
        in_specs=[VMEM] * groups,
        out_specs=VMEM,
        compiler_params=params,
        name="pool",
    )(*packs)
    got = near(swap(pooled))
    copies = pltpu.VMEM((domains * piece, width), BF16)
    mid = pl.pallas_call(
        functools.partial(coarse_mid_kernel, piece=piece, domains=domains),
        out_shape=copies,
        in_specs=[VMEM] * 2,
        out_specs=VMEM,
        compiler_params=params,
        name="coarse_mid",
    )(got, near(coarse_nodes))
    half = groups // 2
    table = pltpu.VMEM((owner_rows * domains // CHUNK // 2, width, CHUNK), BF16)
    ctiles = -(-(coarse_slots + LANES) // ctile)
    csenders = near(coarse_senders[None])
    creceivers = near(coarse_receivers[None])
    cost = pl.CostEstimate(flops=1 << 31, transcendentals=0, bytes_accessed=0)

    def coarse_first(parts):
        return pl.pallas_call(
            functools.partial(coarse_first_kernel, near_parts=half, **sizes),
            out_shape=(pltpu.VMEM((ctiles, width, ctile), BF16), pltpu.VMEM((piece, width), F32)),
            in_specs=[VMEM] * (half + 4),
            out_specs=(VMEM, VMEM),
            scratch_shapes=[table],
            compiler_params=params,
            cost_estimate=cost,
            name="coarse_first",
        )(*parts, far(coarse_edges), csenders, creceivers, w_edge)

    closer, others, (cpre, csome) = spread_over(swap(mid), groups, coarse_first)
    coarse = pl.pallas_call(
        functools.partial(coarse_second_kernel, far_parts=half, **sizes),
        out_shape=copies,
        in_specs=[VMEM] * (half + 8),
        out_specs=VMEM,
        scratch_shapes=[table, pltpu.VMEM((piece, width), F32)],
        compiler_params=params,
        name="coarse_second",
    )(
        closer[0], *others, near(cpre), near(csome), csenders, creceivers, w_edge, w_node, w_out,
    )

    def return_first(parts):
        return pl.pallas_call(
            functools.partial(return_first_kernel, near_parts=half, nodes=nodes, **sizes),
            out_shape=pltpu.VMEM((width, nodes), F32),
            in_specs=[VMEM] * (half + 3),
            out_specs=VMEM,
            scratch_shapes=[table],
            compiler_params=params,
            cost_estimate=cost,
            name="back_first",
        )(*parts, packed, parents, w_node)

    closer, others, pre_out = spread_over(swap(coarse), groups, return_first)
    fine_out, coarse_out = pl.pallas_call(
        functools.partial(return_second_kernel, groups=groups, nodes=nodes, **sizes),
        out_shape=(
            jax.ShapeDtypeStruct((nodes, width), BF16),
            jax.ShapeDtypeStruct((owner_rows, width), BF16),
        ),
        in_specs=[VMEM] * (groups + 5),
        out_specs=(VMEM, VMEM),
        scratch_shapes=[table],
        compiler_params=params,
        name="back_second",
    )(*closer, *others, near(pre_out), packed, parents, w_node, w_out)
    return (fine_out[None], coarse_out)


def solution(mesh):
    placed = (
        P("grp", "dom", None),
        P("grp", "dom", None),
        P("grp", "dom"),
        P("grp", "dom"),
        P("grp", "dom"),
        P("grp", "dom", None),
        P("grp", "dom"),
        P("dom", None),
        P("dom", None),
        P("dom"),
        P("dom"),
        P(),
        P(),
        P(),
    )
    return jax.shard_map(
        per_device,
        mesh=mesh,
        in_specs=placed,
        out_specs=(P("grp", "dom", None), P("dom", None)),
        check_vma=False,
    )
```
